128 devices in a mesh: grp: 2 (over core), seg: 64 (over x, y, z).
Axes of the slice: x: 4, y: 4, z: 4, core: 2. Of those that a mesh axis runs over, the one named last changes fastest.
Arguments:
- coeffs: bfloat16 [858, 32768], P(None, ('grp', 'seg')), may hold values from -6 to 6
- tracer: bfloat16 [286, 32768], P(None, ('grp', 'seg')), may hold values from -6 to 6
- up_op: bfloat16 [168, 858], replicated, may hold values from -0.21875 to 0.21875
- far_ops: bfloat16 [168, 16, 168], replicated, may hold values from -0.005859375 to 0.005859375
- down_op: bfloat16 [858, 168], replicated, may hold values from -0.5 to 0.5
- near_ops: bfloat16 [858, 8, 858], replicated, may hold values from -0.0390625 to 0.0390625
- face_dirs: float32 [3, 8], replicated, may hold values from -4 to 4
- leaf_octant: int32 [32768], P(('grp', 'seg')), may hold values from 0 to 1023, as said below
- far_src: int32 [189, 1024], P(None, ('grp', 'seg')), may hold values from 0 to 1023
- far_type: int32 [189, 1024], P(None, ('grp', 'seg')), may hold values from 0 to 15
- near_list: int32 [27, 32768], P(None, ('grp', 'seg')), may hold values from 0 to 511, as said below
- near_type: int32 [27, 32768], P(None, ('grp', 'seg')), may hold values from 0 to 8, as said below
- new_owner: int32 [32768, 1], P(('grp', 'seg')), may hold values from 0 to 127; in each aligned block of 256 rows (0 to 255, 256 to 511, ...) at most 4 rows name the same one
Outputs:
- moved: bfloat16 [1144, 65536], P(None, ('grp', 'seg'))
The draws below stay inside these ranges and needn't reach their ends.
Inputs may be any that keep to these rules, and one draw needn't show every extreme that they name: `leaf_octant`: never falling along the leaves; every octant holds at least one leaf; octant o begins at leaf 0 for o = 0, else among the 32 leaves that end at leaf o * 32. neighbour[k, l] = (l // 256) * 256 - 128 + near_list[k, l] is a leaf of the same group of devices along seg as leaf l. `near_type`: the value 8 marks an empty slot. `new_owner`: among the 256 leaves of one device, at most 4 have the same new owner.
All inputs are finite; a program needn't handle non-finite values.
Results may differ from the reference program's by a relative error of at most 0.0065.
Values may be sent and summed in bfloat16 or wider, within the bound.
A program may use at most 128 MiB of HBM per device.

```python
import math
import jax
import jax.numpy as jnp
import numpy as np
from jax import lax

NCOEF = 286
COMP = 3
COEF = 858
MULT = 168
NTYPES = 8
NEAR_K = 27
FTYPES = 16
FAR_K = 189
LEAF_DEV = 256
HALO = 128
OCT_DEV = 8
OCTANTS = 1024
LEAVES = 32768
CAP = 4
N_SEG = 64
DEVICES = 128


def draw_leaf_octant(key, part):
    spacing = LEAF_DEV // OCT_DEV
    jitter = jax.random.randint(jax.random.fold_in(key, 21), (OCTANTS,), 0, spacing)
    jitter = jnp.where(jnp.arange(OCTANTS, dtype=jnp.int32) == 0, 0, jitter)
    starts = (jnp.arange(OCTANTS, dtype=jnp.int32) * spacing - jitter).astype(jnp.int32)
    leaf_ids = jnp.arange(LEAVES, dtype=jnp.int32)
    found = jnp.searchsorted(starts, leaf_ids, side='right') - 1
    return found.astype(jnp.int32)


def near_pair(key):
    leaf_ids = jnp.arange(LEAVES, dtype=jnp.int32)
    device = leaf_ids // LEAF_DEV
    position = leaf_ids % LEAF_DEV
    segment = device % N_SEG
    lowest = jnp.where(segment == 0, -position, -HALO)
    highest = jnp.where(segment == N_SEG - 1, LEAF_DEV - 1 - position, HALO)
    random_bits = jax.random.randint(jax.random.fold_in(key, 11), (NEAR_K, LEAVES), 0, 1 << 20)
    offset = lowest[None, :] + random_bits % (highest - lowest + 1)[None, :]
    window_place = HALO + position[None, :] + offset
    device_total = LEAVES // LEAF_DEV
    threshold = 45 + 45 * device // max(device_total - 1, 1)
    chance = jax.random.randint(jax.random.fold_in(key, 12), (NEAR_K, LEAVES), 0, 100)
    type_draw = jax.random.randint(jax.random.fold_in(key, 13), (NEAR_K, LEAVES), 0, NTYPES)
    near_kind = jnp.where(chance < threshold[None, :], type_draw, NTYPES)
    return (window_place.astype(jnp.int32), near_kind.astype(jnp.int32))


def draw_near_list(key, part):
    return near_pair(key)[0]


def draw_near_type(key, part):
    return near_pair(key)[1]


def set_ends(result, stream_key, least, top_value):
    spot = [jax.random.randint(jax.random.fold_in(stream_key, axis), (), 0, length) for axis, length in enumerate(result.shape)]
    main_axis = result.shape.index(max(result.shape))
    next_to = spot[:main_axis] + [(spot[main_axis] + 1) % result.shape[main_axis]] + spot[main_axis + 1:]
    return result.at[tuple(spot)].set(least).at[tuple(next_to)].set(top_value)


def steps_of(own_key, dims, pieces, least, high):
    level, own = 1.0, jax.random.fold_in(own_key, 6)
    for dim, blocks in pieces:
        steps = jnp.exp(jax.random.uniform(jax.random.fold_in(own, dim), (blocks,), jnp.float32, least / len(pieces), high / len(pieces)))
        level = level * jnp.repeat(steps, dims[dim] // blocks).reshape([-1 if axis == dim else 1 for axis in range(len(dims))])
    return level


def deal_out(key, own, number, rows, amount, top, most, slope):
    order = jax.random.permutation(key, amount)
    packed, usual = load_shares(amount, rows * top, most, slope, True), load_shares(amount, rows * top, most, slope, False)
    places = jnp.arange(amount)

    def named(lengths, rotation):
        used = int((lengths > 0).sum())
        fixed = max(1, used // 4)
        passed = fixed + (places - fixed + rotation * (used - fixed)) % max(1, amount - fixed)
        return jnp.zeros((amount,), jnp.int32).at[order[jnp.where(places < fixed, places, passed)]].set(jnp.asarray(lengths, jnp.int32))

    lengths = jnp.where(number % 4 == 0, named(packed, number // 4), named(usual, number - number // 4 - 1))
    mixed = jax.random.permutation(jax.random.fold_in(own, 3), amount)
    giver, sink = mixed[0:amount // 2 * 2:2], mixed[1:amount // 2 * 2:2]
    room = jnp.minimum(lengths[giver] - 1, most - lengths[sink]) // 2
    room = jnp.where((giver == order[0]) | (sink == order[0]) | (lengths[sink] == 0), 0, jnp.maximum(room, 0))
    passed = jax.random.randint(jax.random.fold_in(own, 4), (amount // 2,), 0, 1 << 20) % (room + 1)
    lengths = lengths.at[giver].add(-passed).at[sink].add(passed)
    labels = jnp.searchsorted(jnp.cumsum(lengths), jnp.arange(rows * top), side="right").astype(jnp.int32)
    grid = labels.reshape(top, rows).T
    grid = grid[jax.random.permutation(jax.random.fold_in(own, 1), rows)]
    rotation = jax.random.randint(jax.random.fold_in(own, 2), (rows, 1), 0, top)
    return jnp.take_along_axis(grid, (jnp.arange(top)[None, :] + rotation) % top, axis=1)


def load_shares(number_of, total, limit, slope, full):
    loads = [(1 << 20) // math.isqrt(grade ** slope) + 1 for grade in range(1, number_of + 1)]
    largest = limit if full else min(limit, max(-(-total // number_of), total * loads[0] // sum(loads)))
    least = 1 if total - largest >= number_of - 1 else 0
    given, rest = [largest] + [least] * (number_of - 1), total - largest - least * (number_of - 1)
    while rest > 0:
        candidates = [i for i in range(1, number_of) if given[i] < largest] or [i for i in range(1, number_of) if given[i] < limit]
        mass, left = sum([loads[i] for i in candidates]), rest
        for i in candidates:
            extra = min(limit - given[i], max(1, left * loads[i] // mass), rest)
            given[i] = given[i] + extra
            rest = rest - extra
    return np.array(given)


def scatter_about(stream_key, shape, deviation, bound, split=(), kind=jnp.bfloat16):
    values = deviation * jax.random.normal(stream_key, shape, jnp.float32)
    if split:
        values = values * steps_of(stream_key, shape, split, -0.22, 0.18)
    return jnp.clip(values, -bound, bound).astype(kind)


def setup_inputs(seed: int = 0) -> dict:
    streams_of = jax.random.split(jax.random.key(seed), 14)
    coeffs = scatter_about(streams_of[0], (COEF, LEAVES), 1.0, 6.0, ((1, 128),))
    tracer = scatter_about(streams_of[1], (NCOEF, LEAVES), 1.0, 6.0, ((1, 128),))
    up_op = scatter_about(streams_of[2], (MULT, COEF), COEF ** -0.5, 0.21875)
    far_ops = scatter_about(streams_of[3], (MULT, FTYPES, MULT), (MULT * FAR_K * (LEAF_DEV // OCT_DEV)) ** -0.5, 0.005859375)
    down_op = scatter_about(streams_of[4], (COEF, MULT), MULT ** -0.5, 0.5)
    near_ops = scatter_about(streams_of[5], (COEF, NTYPES, COEF), (COEF * NEAR_K) ** -0.5, 0.0390625)
    face_dirs = scatter_about(streams_of[6], (COMP, NTYPES), 1.0, 4.0, (), jnp.float32)
    leaf_octant = draw_leaf_octant(jax.random.fold_in(streams_of[13], 71), 0)
    far_src = set_ends(jax.random.randint(streams_of[8], (FAR_K, OCTANTS), 0, OCTANTS), jax.random.fold_in(streams_of[8], 1), 0, OCTANTS - 1).astype(jnp.int32)
    far_type = set_ends(jax.random.randint(streams_of[9], (FAR_K, OCTANTS), 0, FTYPES), jax.random.fold_in(streams_of[9], 1), 0, FTYPES - 1).astype(jnp.int32)
    near_list = draw_near_list(jax.random.fold_in(streams_of[13], 71), 0)
    near_type = draw_near_type(jax.random.fold_in(streams_of[13], 71), 0)
    new_owner_keys = jax.random.split(jax.random.fold_in(streams_of[12], 1), LEAVES // LEAF_DEV)
    new_owner_turns = jax.random.permutation(jax.random.fold_in(streams_of[12], 3), LEAVES // LEAF_DEV)
    new_owner = jax.vmap(lambda own, number: deal_out(jax.random.fold_in(streams_of[12], 2), own, number, LEAF_DEV, DEVICES, 1, CAP, 2))(new_owner_keys, new_owner_turns).reshape((LEAVES, 1))
    return {"coeffs": coeffs, "tracer": tracer, "up_op": up_op, "far_ops": far_ops, "down_op": down_op, "near_ops": near_ops, "face_dirs": face_dirs, "leaf_octant": leaf_octant, "far_src": far_src, "far_type": far_type, "near_list": near_list, "near_type": near_type, "new_owner": new_owner}


def octant_column(octant, per_device, devices):
    block = octant // per_device
    owner = jnp.where(block % 2 == 1, block - 1, (block - devices // 2 - 1) % devices)
    return (owner * per_device + octant % per_device).astype(jnp.int32)


def reference(coeffs, tracer, up_op, far_ops, down_op, near_ops, face_dirs, leaf_octant, far_src, far_type, near_list, near_type, new_owner):
    leaf_ids = jnp.arange(LEAVES, dtype=jnp.int32)
    block_start = ((leaf_ids // LEAF_DEV) * LEAF_DEV).astype(jnp.int32)
    neighbour = (block_start[None, :] - HALO + near_list).astype(jnp.int32)
    leaf_column = octant_column(leaf_octant, OCT_DEV, DEVICES)
    source_column = octant_column(far_src, OCT_DEV, DEVICES)
    leaf_pole = jnp.dot(up_op, coeffs, preferred_element_type=jnp.float32).astype(jnp.bfloat16)
    octant_sum = jax.ops.segment_sum(leaf_pole.astype(jnp.float32).T, leaf_column, num_segments=OCTANTS).T
    octant_pole = octant_sum.astype(jnp.bfloat16)
    picked = jnp.take(octant_pole, source_column.reshape(-1), axis=1).reshape(MULT, FAR_K, OCTANTS)
    type_table = (far_type[:, :, None] == jnp.arange(FTYPES, dtype=jnp.int32)[None, None, :]).astype(jnp.float32)
    grouped = jnp.einsum("cko,kot->tco", picked.astype(jnp.float32), type_table, precision=lax.Precision.HIGHEST).astype(jnp.bfloat16)
    local_exp = jnp.dot(far_ops.reshape(MULT, FTYPES * MULT), grouped.reshape(FTYPES * MULT, OCTANTS), preferred_element_type=jnp.float32).astype(jnp.bfloat16)
    far_field = jnp.dot(down_op, jnp.take(local_exp, leaf_column, axis=1), preferred_element_type=jnp.float32)
    near_field = jnp.zeros((COEF, LEAVES), jnp.float32)
    for type_index in range(NTYPES):
        images = jnp.dot(near_ops[:, type_index, :], coeffs, preferred_element_type=jnp.float32).astype(jnp.bfloat16)

        def add_slot(slot_index, running, images=images, type_index=type_index):
            columns = jnp.take(images, neighbour[slot_index], axis=1).astype(jnp.float32)
            return running + jnp.where((near_type[slot_index] == type_index)[None, :], columns, jnp.zeros((), jnp.float32))

        near_field = lax.fori_loop(0, NEAR_K, add_slot, near_field)
    velocity = near_field + far_field
    speeds = velocity[::NCOEF]
    normal_speed = face_dirs[0][:, None] * speeds[0][None, :] + face_dirs[1][:, None] * speeds[1][None, :] + face_dirs[2][:, None] * speeds[2][None, :]
    live_slot = near_type < NTYPES
    kind_index = jnp.clip(near_type, 0, NTYPES - 1).astype(jnp.int32)
    inflow = jnp.where(live_slot, jnp.maximum(jnp.take_along_axis(normal_speed, kind_index, axis=0), 0.0), 0.0)
    denominator = 1.0 + jnp.sum(inflow, axis=0)
    weights = inflow / denominator[None, :]
    retained = 1.0 - jnp.sum(weights, axis=0)

    def mix_slot(slot_index, running):
        columns = jnp.take(tracer, neighbour[slot_index], axis=1).astype(jnp.float32)
        return running + weights[slot_index][None, :] * columns

    blended = lax.fori_loop(0, NEAR_K, mix_slot, tracer.astype(jnp.float32) * retained[None, :])
    payload = jnp.concatenate([velocity.astype(jnp.bfloat16), blended.astype(jnp.bfloat16)], axis=0)
    owner_rows = new_owner[:, 0].reshape(DEVICES, LEAF_DEV).astype(jnp.int32)
    owner_hot = (owner_rows[:, :, None] == jnp.arange(DEVICES, dtype=jnp.int32)[None, None, :]).astype(jnp.int32)
    slot_rank = (jnp.sum(jnp.cumsum(owner_hot, axis=1).astype(jnp.int32) * owner_hot, axis=2) - 1).astype(jnp.int32)
    source = jnp.arange(DEVICES, dtype=jnp.int32)[:, None]
    column = (owner_rows * (DEVICES * CAP) + source * CAP + slot_rank).reshape(-1).astype(jnp.int32)
    moved = jnp.zeros((COEF + NCOEF, DEVICES * DEVICES * CAP), jnp.bfloat16).at[:, column].set(payload)
    return moved
```

```python
import functools

import jax
import jax.numpy as jnp
from jax import lax
from jax.experimental import pallas as pl
from jax.experimental.pallas import tpu as pltpu
from jax.sharding import PartitionSpec as P

NCOEF = 286
COEF = 858
MULT = 168
NTYPES = 8
NEAR_K = 27
FTYPES = 16
FAR_K = 189
LEAF = 256
HALO = 128
OCT_DEV = 8
OCTANTS = 1024
CAP = 4
SEG = 64
DEV = 128
KPAD = 896
OBLK = 32
NBLK = 27
HALF = 576
MSG = 640
GRP_SEG = ("grp", "seg")
LOGICAL = pl.DeviceIdType.LOGICAL
BF = jnp.bfloat16
F32 = jnp.float32
I32 = jnp.int32
VMEM = pltpu.VMEM


def dot(a, b, ca=1, cb=0):
    return lax.dot_general(a, b, (((ca,), (cb,)), ((), ())), preferred_element_type=F32)


def hot(mask):
    return jnp.where(mask, 1.0, 0.0).astype(BF)


def iota(shape, dim):
    return lax.broadcasted_iota(I32, shape, dim)


def remote(src, dst, send_sem, recv_sem, device):
    return pltpu.make_async_remote_copy(
        src_ref=src,
        dst_ref=dst,
        send_sem=send_sem,
        recv_sem=recv_sem,
        device_id=device,
        device_id_type=LOGICAL,
    )


def step_kernel(
    coeffs,
    tracer,
    up_op,
    far_ops,
    down_op,
    near_ops,
    face_dirs,
    leaf_octant,
    far_src,
    far_type,
    near_list,
    near_type,
    new_owner,
    arrived,
    raw_ops,
    ops,
    counts,
    group,
    mixed,
    halo_coeffs,
    halo_tracer,
    poles,
    far_count,
    local_own,
    local_in,
    local_edge,
    place,
    velocity,
    outgoing,
    slots,
    load_sem,
    halo_send,
    halo_recv,
    pole_send,
    pole_recv,
    pair_send,
    pair_recv,
    local_send,
    local_recv,
    move_send,
    move_recv,
):
    grp = lax.axis_index("grp")
    seg = lax.axis_index("seg")
    me = grp * SEG + seg
    partner = (1 - grp) * SEG + seg

    barrier = pltpu.get_barrier_semaphore()

    def greet(j, carry):
        pl.semaphore_signal(
            barrier, inc=1, device_id=lax.rem(me + j, DEV), device_id_type=LOGICAL
        )
        return carry

    lax.fori_loop(1, DEV, greet, 0)
    rows = COEF * NTYPES
    load = pltpu.make_async_copy(near_ops, raw_ops.at[pl.ds(0, rows)], load_sem)
    load.start()

    leaf_pole = dot(up_op[...], coeffs[...]).astype(BF)
    piece = hot(iota((16, LEAF), 0) == leaf_octant[...] - me * OCT_DEV)
    poles[pl.ds(me, 1)] = jnp.zeros((1, 16, 256), BF)
    poles[pl.ds(me, 1), :, 0:MULT] = dot(piece, leaf_pole, 1, 1).astype(BF)[None]
    pl.semaphore_wait(barrier, DEV - 1)

    def send_pole(j, carry):
        there = grp * SEG + lax.rem(seg + j, SEG)
        remote(poles.at[me], poles.at[me], pole_send, pole_recv, there).start()
        return carry

    lax.fori_loop(1, SEG, send_pole, 0)
    right = grp * SEG + lax.rem(seg + 1, SEG)
    left = grp * SEG + lax.rem(seg + SEG - 1, SEG)
    low = pl.ds(0, HALO)
    high = pl.ds(HALO, HALO)
    halos = [
        remote(coeffs.at[:, high], halo_coeffs.at[:, low], halo_send.at[0], halo_recv.at[0], right),
        remote(coeffs.at[:, low], halo_coeffs.at[:, high], halo_send.at[1], halo_recv.at[1], left),
        remote(tracer.at[:, high], halo_tracer.at[:, low], halo_send.at[2], halo_recv.at[2], right),
        remote(tracer.at[:, low], halo_tracer.at[:, high], halo_send.at[3], halo_recv.at[3], left),
    ]
    for copy in halos:
        copy.start()

    listed = near_list[...]
    inside = (listed >= HALO) & (listed < HALO + LEAF)
    spot = jnp.where(inside, listed - HALO, jnp.where(listed < HALO, listed + LEAF, listed))
    kind = near_type[...]
    one = jnp.ones_like(kind)
    first_word = jnp.where(kind < 4, one << (8 * jnp.minimum(kind, 3)), 0)
    other_word = jnp.where(
        (kind >= 4) & (kind < NTYPES), one << (8 * (jnp.clip(kind, 4, 7) - 4)), 0
    )
    slots[0] = spot
    slots[1] = first_word
    slots[2] = other_word

    def count_rows(block, carry):
        base = pl.multiple_of(block * 32, 32)
        place_of = iota((32, LEAF), 0) + base
        first = jnp.zeros((32, LEAF), I32)
        other = jnp.zeros((32, LEAF), I32)
        for k in range(NEAR_K):
            here = place_of == slots[0, k : k + 1, :]
            first = first + jnp.where(here, slots[1, k : k + 1, :], 0)
            other = other + jnp.where(here, slots[2, k : k + 1, :], 0)
        for t in range(NTYPES):
            word = first if t < 4 else other
            value = lax.shift_right_logical(word, jnp.full_like(word, 8 * (t % 4))) & 255
            counts[t, pl.ds(base, 32), :] = value.astype(F32).astype(BF)
        return carry

    lax.fori_loop(0, 16, count_rows, 0)

    for c in range(OCT_DEV):
        source = hot(iota((FAR_K, OCTANTS), 1) == far_src[:, c : c + 1])
        kind_hot = hot(iota((FAR_K, FTYPES), 1) == far_type[:, c : c + 1])
        far_count[c * FTYPES : (c + 1) * FTYPES, :] = dot(kind_hot, source, 0, 0).astype(BF)

    owner = new_owner[...].astype(F32)
    leaf_row = iota((LEAF, LEAF), 0)
    leaf_col = iota((LEAF, LEAF), 1)
    owner_row = jnp.sum(jnp.where(leaf_row == leaf_col, owner, 0.0), axis=0, keepdims=True)
    before = (leaf_row < leaf_col) & (owner == owner_row)
    rank = jnp.sum(jnp.where(before, 1.0, 0.0), axis=0, keepdims=True)
    target = (owner_row * 8.0 + rank).astype(I32)

    def place_rows(block, carry):
        base = pl.multiple_of(block * 256, 256)
        row = iota((256, LEAF), 0) + base
        place[0, pl.ds(base, 256), :] = hot(row == target)
        place[1, pl.ds(base, 256), :] = hot(row == target + CAP)
        return carry

    lax.fori_loop(0, 4, place_rows, 0)

    raw_ops[rows : NBLK * 256, :] = jnp.zeros((NBLK * 256 - rows, COEF), BF)
    for t in range(NTYPES):
        ops[:, t * KPAD + 768 : (t + 1) * KPAD] = jnp.zeros((NBLK * OBLK, 128), BF)
        group[t * KPAD + 848 : (t + 1) * KPAD, :] = jnp.zeros((48, LEAF), BF)
    turn_row = iota((256, 256), 0)
    turn = hot(iota((256, 256), 1) == lax.rem(turn_row, OBLK) * NTYPES + turn_row // OBLK)
    load.wait()

    def turn_block(b, carry):
        block = raw_ops[pl.ds(pl.multiple_of(b * 256, 256), 256), :]
        turned = dot(turn, block).astype(BF)
        out_rows = pl.ds(pl.multiple_of(b * OBLK, OBLK), OBLK)
        for t in range(NTYPES):
            ops[out_rows, t * KPAD : t * KPAD + COEF] = turned[t * OBLK : (t + 1) * OBLK, :]
        return carry

    lax.fori_loop(0, NBLK, turn_block, 0)

    remote(
        poles.at[pl.ds(0, SEG - 1)], poles.at[pl.ds(0, SEG - 1)], pole_send, pole_recv, partner
    ).wait_recv()
    mine = poles.at[pl.ds(grp * SEG, SEG)]
    pair = remote(mine, mine, pair_send, pair_recv, partner)
    pair.start()

    for copy in halos:
        copy.wait_recv()

    def gather_kind(t, carry):
        own = counts[t, 0:LEAF, :]
        edge = counts[t, LEAF : 2 * LEAF, :]
        base = pl.multiple_of(t * KPAD, KPAD)
        total = dot(coeffs[...], own) + dot(halo_coeffs[...], edge)
        group[pl.ds(base, COEF), :] = total.astype(BF)
        mixed[t] = dot(tracer[...], own) + dot(halo_tracer[...], edge)
        return carry

    lax.fori_loop(0, NTYPES, gather_kind, 0)

    pair.wait_recv()
    every = poles[...].astype(F32)
    edge_pole = every[:, 8:9, :]
    moved_edge = jnp.concatenate([jnp.zeros((1, 1, 256), F32), edge_pole[: DEV - 1]], axis=0)
    octant_pole = every[:, 0:8, :] + jnp.where(iota((DEV, 8, 256), 1) == 0, moved_edge, 0.0)
    octant_pole = octant_pole.reshape(OCTANTS, 256).astype(BF)
    grouped = dot(far_count[...], octant_pole).astype(BF)[:, 0:MULT]
    shifted = dot(far_ops[...], grouped, 1, 1).reshape(MULT, FTYPES, 128)
    same = lax.rem(iota((1, FTYPES, 128), 2), FTYPES) == iota((1, FTYPES, 128), 1)
    by_kind = jnp.sum(jnp.where(same, shifted, 0.0), axis=1).astype(BF)
    fold = hot(iota((16, 128), 1) // FTYPES == iota((16, 128), 0))
    local_own[...] = jnp.zeros((16, 256), BF)
    local_own[:, 0:MULT] = dot(fold, by_kind, 1, 1).astype(BF)
    holder = jnp.where(lax.rem(me, 2) == 0, me + 1, lax.rem(me + SEG + 1, DEV))
    to_holder = remote(local_own, local_in, local_send.at[0], local_recv.at[0], holder)
    to_holder.start()
    to_pair = remote(local_own, local_edge, local_send.at[1], local_recv.at[1], partner)
    to_pair.start()

    def near_rows(block, carry):
        here = pl.ds(pl.multiple_of(block * 288, 32), 288)
        velocity[here, :] = dot(ops[here, :], group[...])
        return carry

    lax.fori_loop(0, 3, near_rows, 0)

    to_holder.wait_recv()
    to_pair.wait_recv()
    row = iota((16, 256), 0)
    from_own = local_own[...].astype(F32)[0:1, :]
    from_pair = local_edge[...].astype(F32)[0:1, :]
    even = lax.rem(jnp.full((1, 256), me, I32), 2) == 0
    ninth = jnp.where(even, from_own, from_pair)
    nine = jnp.where(row < 8, local_in[...].astype(F32), jnp.where(row == 8, ninth, 0.0))
    leaf_local = dot(nine.astype(BF)[:, 0:MULT], piece, 0, 0).astype(BF)
    speed = velocity[0:COEF, :] + dot(down_op[...], leaf_local)

    flows = []
    total_in = jnp.zeros((1, LEAF), F32)
    for t in range(NTYPES):
        normal = (
            face_dirs[0, t] * speed[0:1, :]
            + face_dirs[1, t] * speed[NCOEF : NCOEF + 1, :]
            + face_dirs[2, t] * speed[2 * NCOEF : 2 * NCOEF + 1, :]
        )
        number = jnp.sum(jnp.where(kind == t, 1.0, 0.0), axis=0, keepdims=True)
        flow = jnp.maximum(normal, 0.0)
        flows.append((flow, number))
        total_in = total_in + flow * number
    denominator = 1.0 + total_in
    kept = jnp.ones((1, LEAF), F32)
    blended = jnp.zeros((NCOEF, LEAF), F32)
    for t, (flow, number) in enumerate(flows):
        weight = flow / denominator
        kept = kept - weight * number
        blended = blended + mixed[t] * weight
    blended = blended + tracer[...].astype(F32) * kept

    upper = speed[0:HALF, :].astype(BF)
    lower = jnp.concatenate(
        [speed[HALF:COEF, :], blended, jnp.zeros((8, LEAF), F32)], axis=0
    ).astype(BF)

    def pack_rows(block, carry):
        base = pl.ds(pl.multiple_of(block * 256, 256), 256)
        message = dot(place[0, base, :], upper, 1, 1) + dot(place[1, base, :], lower, 1, 1)
        message = jnp.concatenate([message, jnp.zeros((256, MSG - HALF), F32)], axis=1)
        outgoing[pl.ds(block * 32, 32)] = message.reshape(32, 8, MSG).astype(BF)
        return carry

    lax.fori_loop(0, 4, pack_rows, 0)

    def send_rows(j, carry):
        there = lax.rem(me + j, DEV)
        remote(outgoing.at[there], arrived.at[me], move_send, move_recv, there).start()
        return carry

    lax.fori_loop(1, DEV, send_rows, 0)
    arrived[pl.ds(me, 1)] = outgoing[pl.ds(me, 1)]

    for copy in halos:
        copy.wait_send()
    many = pl.ds(0, SEG - 1)
    remote(poles.at[many], poles.at[many], pole_send, pole_recv, partner).wait_send()
    pair.wait_send()
    to_holder.wait_send()
    to_pair.wait_send()
    most = pl.ds(0, DEV - 1)
    last = remote(outgoing.at[most], arrived.at[most], move_send, move_recv, partner)
    last.wait_send()
    last.wait_recv()


def step(*args):
    (
        coeffs,
        tracer,
        up_op,
        far_ops,
        down_op,
        near_ops,
        face_dirs,
        leaf_octant,
        far_src,
        far_type,
        near_list,
        near_type,
        new_owner,
    ) = args
    whole = pl.BlockSpec(memory_space=VMEM)
    dma = pltpu.SemaphoreType.DMA
    return pl.pallas_call(
        step_kernel,
        name="step",
        out_shape=jax.ShapeDtypeStruct((DEV, 8, MSG), BF),
        in_specs=[whole] * 5
        + [pl.BlockSpec(memory_space=pl.ANY), pl.BlockSpec(memory_space=pltpu.SMEM)]
        + [whole] * 6,
        out_specs=whole,
        scratch_shapes=[
            VMEM((NBLK * 256, COEF), BF),
            VMEM((NBLK * OBLK, NTYPES * KPAD), BF),
            VMEM((NTYPES, 2 * LEAF, LEAF), BF),
            VMEM((NTYPES * KPAD, LEAF), BF),
            VMEM((NTYPES, NCOEF, LEAF), F32),
            VMEM((COEF, LEAF), BF),
            VMEM((NCOEF, LEAF), BF),
            VMEM((DEV, 16, 256), BF),
            VMEM((128, OCTANTS), BF),
            VMEM((16, 256), BF),
            VMEM((16, 256), BF),
            VMEM((16, 256), BF),
            VMEM((2, 1024, LEAF), BF),
            VMEM((NBLK * OBLK, LEAF), F32),
            VMEM((DEV, 8, MSG), BF),
            VMEM((3, NEAR_K, LEAF), I32),
            dma,
            dma((4,)),
            dma((4,)),
            dma,
            dma,
            dma,
            dma,
            dma((2,)),
            dma((2,)),
            dma,
            dma,
        ],
        compiler_params=pltpu.CompilerParams(
            collective_id=0, has_side_effects=True, vmem_limit_bytes=64_000_000
        ),
    )(
        coeffs,
        tracer,
        up_op,
        far_ops.reshape(MULT * FTYPES, MULT),
        down_op,
        near_ops.reshape(COEF * NTYPES, COEF),
        face_dirs,
        leaf_octant.reshape(1, LEAF),
        far_src,
        far_type,
        near_list,
        near_type,
        new_owner,
    )


def turn_kernel(arrived, moved):
    block = arrived[...].astype(F32).reshape(256, MSG).astype(BF)
    row = iota((256, 256), 0)
    col = iota((256, 256), 1)
    wanted = (row // 8) * CAP + lax.rem(row, CAP) + 128 * (lax.rem(row, 8) // CAP)
    turned = dot(block, hot(col == wanted), 0, 0).astype(BF)
    moved[0:HALF, :] = turned[0:HALF, 0:128]
    moved[HALF : COEF + NCOEF, :] = turned[0 : COEF + NCOEF - HALF, 128:256]


def turned_rows(arrived):
    return pl.pallas_call(
        turn_kernel,
        name="turn",
        grid=(4,),
        out_shape=jax.ShapeDtypeStruct((COEF + NCOEF, DEV * CAP), BF),
        in_specs=[pl.BlockSpec((32, 8, MSG), lambda g: (g, 0, 0))],
        out_specs=pl.BlockSpec((COEF + NCOEF, 128), lambda g: (0, g)),
        compiler_params=pltpu.CompilerParams(dimension_semantics=("arbitrary",)),
    )(arrived)


def local(*args):
    return turned_rows(step(*args))


def solution(mesh):
    split = P(None, GRP_SEG)
    in_specs = (
        split,
        split,
        P(),
        P(),
        P(),
        P(),
        P(),
        P(GRP_SEG),
        split,
        split,
        split,
        split,
        P(GRP_SEG, None),
    )
    return jax.shard_map(local, mesh=mesh, in_specs=in_specs, out_specs=split, check_vma=False)
```

```python
import functools

import jax
import jax.numpy as jnp
from jax import lax
from jax.experimental import pallas as pl
from jax.experimental.pallas import tpu as pltpu
from jax.sharding import PartitionSpec as P

NCOEF = 286
COEF = 858
MULT = 168
NTYPES = 8
NEAR_K = 27
FTYPES = 16
FAR_K = 189
LEAF = 256
HALO = 128
OCT_DEV = 8
OCTANTS = 1024
CAP = 4
SEG = 64
DEV = 128
KPAD = 896
OBLK = 32
NBLK = 27
FRONT = 640
BACK = 512
REST = 504
GRP_SEG = ("grp", "seg")
LOGICAL = pl.DeviceIdType.LOGICAL
BF = jnp.bfloat16
F32 = jnp.float32
I32 = jnp.int32
VMEM = pltpu.VMEM


def dot(a, b, ca=1, cb=0):
    return lax.dot_general(a, b, (((ca,), (cb,)), ((), ())), preferred_element_type=F32)


def hot(mask):
    return jnp.where(mask, 1.0, 0.0).astype(BF)


def iota(shape, dim):
    return lax.broadcasted_iota(I32, shape, dim)


def remote(src, dst, send_sem, recv_sem, device):
    return pltpu.make_async_remote_copy(
        src_ref=src,
        dst_ref=dst,
        send_sem=send_sem,
        recv_sem=recv_sem,
        device_id=device,
        device_id_type=LOGICAL,
    )


def step_kernel(
    coeffs_hbm,
    tracer_hbm,
    up_hbm,
    far_hbm,
    down_hbm,
    near_hbm,
    face_dirs,
    octant_hbm,
    source_hbm,
    type_hbm,
    list_hbm,
    kind_hbm,
    owner_hbm,
    arrived_front,
    arrived_back,
    window,
    tracers,
    up_op,
    far_ops,
    down_op,
    leaf_octant,
    far_src,
    far_type,
    near_list,
    near_type,
    new_owner,
    raw_ops,
    ops,
    counts,
    group,
    mixed,
    poles,
    far_count,
    local_own,
    local_in,
    local_edge,
    place,
    velocity,
    front,
    back,
    slots,
    load_sem,
    halo_send,
    halo_recv,
    pole_send,
    pole_recv,
    pair_send,
    pair_recv,
    local_send,
    local_recv,
    move_send,
    move_recv,
):
    grp = lax.axis_index("grp")
    seg = lax.axis_index("seg")
    me = grp * SEG + seg
    partner = (1 - grp) * SEG + seg
    own_lanes = pl.ds(0, LEAF)
    rows = COEF * NTYPES

    def load(source, target, k):
        copy = pltpu.make_async_copy(source, target, load_sem.at[k])
        copy.start()
        return copy

    loads = [
        load(coeffs_hbm, window.at[:, own_lanes], 0),
        load(up_hbm, up_op, 1),
        load(octant_hbm, leaf_octant, 2),
        load(list_hbm, near_list, 3),
        load(kind_hbm, near_type, 4),
        load(source_hbm, far_src, 5),
        load(type_hbm, far_type, 6),
        load(owner_hbm, new_owner, 7),
        load(tracer_hbm, tracers.at[:, own_lanes], 8),
        load(near_hbm, raw_ops.at[pl.ds(0, rows)], 9),
        load(far_hbm, far_ops, 10),
        load(down_hbm, down_op, 11),
    ]

    barrier = pltpu.get_barrier_semaphore()

    def greet(j, carry):
        there = grp * SEG + lax.rem(seg + j, SEG)
        pl.semaphore_signal(barrier, inc=1, device_id=there, device_id_type=LOGICAL)
        return carry

    lax.fori_loop(1, SEG, greet, 0)
    pl.semaphore_signal(barrier, inc=1, device_id=partner, device_id_type=LOGICAL)

    for copy in loads[0:3]:
        copy.wait()
    leaf_pole = dot(up_op[...], window[:, 0:LEAF]).astype(BF)
    piece = hot(iota((16, LEAF), 0) == leaf_octant[...] - me * OCT_DEV)
    poles[pl.ds(me, 1)] = jnp.zeros((1, 16, 256), BF)
    poles[pl.ds(me, 1), :, 0:MULT] = dot(piece, leaf_pole, 1, 1).astype(BF)[None]

    for copy in loads[3:9]:
        copy.wait()
    listed = near_list[...]
    inside = (listed >= HALO) & (listed < HALO + LEAF)
    spot = jnp.where(inside, listed - HALO, jnp.where(listed < HALO, listed + LEAF, listed))
    kind = near_type[...]
    one = jnp.ones_like(kind)
    first_word = jnp.where(kind < 4, one << (8 * jnp.minimum(kind, 3)), 0)
    other_word = jnp.where(
        (kind >= 4) & (kind < NTYPES), one << (8 * (jnp.clip(kind, 4, 7) - 4)), 0
    )
    slots[0] = spot
    slots[1] = first_word
    slots[2] = other_word

    def count_rows(block, carry):
        base = pl.multiple_of(block * 32, 32)
        place_of = iota((32, LEAF), 0) + base
        first = jnp.zeros((32, LEAF), I32)
        other = jnp.zeros((32, LEAF), I32)
        for k in range(NEAR_K):
            here = place_of == slots[0, k : k + 1, :]
            first = first + jnp.where(here, slots[1, k : k + 1, :], 0)
            other = other + jnp.where(here, slots[2, k : k + 1, :], 0)
        for t in range(NTYPES):
            word = first if t < 4 else other
            value = lax.shift_right_logical(word, jnp.full_like(word, 8 * (t % 4))) & 255
            counts[t, pl.ds(base, 32), :] = value.astype(F32).astype(BF)
        return carry

    lax.fori_loop(0, 16, count_rows, 0)

    pl.semaphore_wait(barrier, SEG)

    def send_pole(j, carry):
        there = grp * SEG + lax.rem(seg + j, SEG)
        remote(poles.at[me], poles.at[me], pole_send, pole_recv, there).start()
        return carry

    right = grp * SEG + lax.rem(seg + 1, SEG)
    left = grp * SEG + lax.rem(seg + SEG - 1, SEG)
    low = pl.ds(0, HALO)
    high = pl.ds(HALO, HALO)
    to_low = pl.ds(LEAF, HALO)
    to_high = pl.ds(LEAF + HALO, HALO)
    halos = [
        remote(src.at[:, lanes], src.at[:, there], halo_send.at[k], halo_recv.at[k], device)
        for k, (src, lanes, there, device) in enumerate(
            (
                (window, high, to_low, right),
                (window, low, to_high, left),
                (tracers, high, to_low, right),
                (tracers, low, to_high, left),
            )
        )
    ]
    lax.fori_loop(1, SEG, send_pole, 0)
    for copy in halos:
        copy.start()

    for c in range(OCT_DEV):
        source = hot(iota((OCTANTS, FAR_K), 0) == far_src[c : c + 1, :])
        kind_hot = hot(iota((FTYPES, FAR_K), 0) == far_type[c : c + 1, :])
        far_count[c * FTYPES : (c + 1) * FTYPES, :] = dot(kind_hot, source, 1, 1).astype(BF)

    owner_row = new_owner[...].astype(F32)
    leaf_row = iota((LEAF, LEAF), 0)
    leaf_col = iota((LEAF, LEAF), 1)
    owner = jnp.sum(jnp.where(leaf_row == leaf_col, owner_row, 0.0), axis=1, keepdims=True)
    before = (leaf_row < leaf_col) & (owner == owner_row)
    rank = jnp.sum(jnp.where(before, 1.0, 0.0), axis=0, keepdims=True)
    target = (owner_row * float(CAP) + rank).astype(I32)
    place[...] = hot(iota((DEV * CAP, LEAF), 0) == target)

    raw_ops[rows : NBLK * 256, :] = jnp.zeros((NBLK * 256 - rows, COEF), BF)
    for t in range(NTYPES):
        ops[:, t * KPAD + 768 : (t + 1) * KPAD] = jnp.zeros((NBLK * OBLK, 128), BF)
        group[t * KPAD + 848 : (t + 1) * KPAD, :] = jnp.zeros((48, LEAF), BF)
    turn_row = iota((256, 256), 0)
    turn = hot(iota((256, 256), 1) == lax.rem(turn_row, OBLK) * NTYPES + turn_row // OBLK)
    for copy in loads[9:12]:
        copy.wait()

    def turn_blocks(b, carry):
        for part in range(3):
            at = b * 3 + part
            block = raw_ops[pl.ds(pl.multiple_of(at * 256, 256), 256), :]
            turned = dot(turn, block).astype(BF)
            out_rows = pl.ds(pl.multiple_of(at * OBLK, OBLK), OBLK)
            for t in range(NTYPES):
                ops[out_rows, t * KPAD : t * KPAD + COEF] = turned[t * OBLK : (t + 1) * OBLK, :]
        return carry

    lax.fori_loop(0, 6, turn_blocks, 0)

    many = pl.ds(0, SEG - 1)
    all_poles = remote(poles.at[many], poles.at[many], pole_send, pole_recv, partner)
    all_poles.wait_recv()
    mine = poles.at[pl.ds(grp * SEG, SEG)]
    pair = remote(mine, mine, pair_send, pair_recv, partner)
    pair.start()
    lax.fori_loop(6, 9, turn_blocks, 0)

    for copy in halos:
        copy.wait_recv()

    def gather_kinds(pair_of, carry):
        for part in range(2):
            t = pair_of * 2 + part
            base = pl.multiple_of(t * KPAD, KPAD)
            group[pl.ds(base, COEF), :] = dot(window[...], counts[t]).astype(BF)
            mixed[t] = dot(tracers[...], counts[t])
        return carry

    lax.fori_loop(0, NTYPES // 2, gather_kinds, 0)

    pair.wait_recv()
    every = poles[...].astype(F32)
    edge_pole = every[:, 8:9, :]
    moved_edge = jnp.concatenate([jnp.zeros((1, 1, 256), F32), edge_pole[: DEV - 1]], axis=0)
    octant_pole = every[:, 0:8, :] + jnp.where(iota((DEV, 8, 256), 1) == 0, moved_edge, 0.0)
    octant_pole = octant_pole.reshape(OCTANTS, 256).astype(BF)
    grouped = dot(far_count[...], octant_pole).astype(BF)[:, 0:MULT]
    shifted = dot(far_ops[...], grouped, 1, 1).reshape(MULT, FTYPES, 128)
    same = lax.rem(iota((1, FTYPES, 128), 2), FTYPES) == iota((1, FTYPES, 128), 1)
    by_kind = jnp.sum(jnp.where(same, shifted, 0.0), axis=1).astype(BF)
    fold = hot(iota((16, 128), 1) // FTYPES == iota((16, 128), 0))
    local_own[...] = jnp.zeros((16, 256), BF)
    local_own[:, 0:MULT] = dot(fold, by_kind, 1, 1).astype(BF)
    holder = jnp.where(lax.rem(me, 2) == 0, me + 1, lax.rem(me + SEG + 1, DEV))
    to_holder = remote(local_own, local_in, local_send.at[0], local_recv.at[0], holder)
    to_holder.start()
    to_pair = remote(local_own, local_edge, local_send.at[1], local_recv.at[1], partner)
    to_pair.start()

    def near_rows(block, carry):
        here = pl.ds(pl.multiple_of(block * 320, 32), 320)
        velocity[here, :] = dot(ops[here, :], group[...])
        return carry

    lax.fori_loop(0, 2, near_rows, 0)

    to_holder.wait_recv()
    to_pair.wait_recv()
    row = iota((16, 256), 0)
    from_own = local_own[...].astype(F32)[0:1, :]
    from_pair = local_edge[...].astype(F32)[0:1, :]
    even = lax.rem(jnp.full((1, 256), me, I32), 2) == 0
    ninth = jnp.where(even, from_own, from_pair)
    nine = jnp.where(row < 8, local_in[...].astype(F32), jnp.where(row == 8, ninth, 0.0))
    leaf_local = dot(nine.astype(BF)[:, 0:MULT], piece, 0, 0).astype(BF)
    velocity[0:FRONT, :] = velocity[0:FRONT, :] + dot(down_op[:, 0:FRONT], leaf_local, 0, 0)

    message = dot(place[...], velocity[0:FRONT, :].astype(BF), 1, 1)
    front[...] = message.reshape(DEV, CAP, FRONT).astype(BF)

    def send_front(j, carry):
        there = lax.rem(me + j, DEV)
        remote(front.at[there], arrived_front.at[me], move_send.at[0], move_recv.at[0], there).start()
        return carry

    lax.fori_loop(1, DEV, send_front, 0)

    rest = dot(ops[FRONT : NBLK * OBLK, :], group[...])[0 : COEF - FRONT, :]
    rest = rest + dot(down_op[:, FRONT:COEF], leaf_local, 0, 0)

    flows = []
    total_in = jnp.zeros((1, LEAF), F32)
    for t in range(NTYPES):
        normal = (
            face_dirs[0, t] * velocity[0:1, :]
            + face_dirs[1, t] * velocity[NCOEF : NCOEF + 1, :]
            + face_dirs[2, t] * velocity[2 * NCOEF : 2 * NCOEF + 1, :]
        )
        number = jnp.sum(jnp.where(kind == t, 1.0, 0.0), axis=0, keepdims=True)
        flow = jnp.maximum(normal, 0.0)
        flows.append((flow, number))
        total_in = total_in + flow * number
    denominator = 1.0 + total_in
    kept = jnp.ones((1, LEAF), F32)
    blended = jnp.zeros((NCOEF, LEAF), F32)
    for t, (flow, number) in enumerate(flows):
        weight = flow / denominator
        kept = kept - weight * number
        blended = blended + mixed[t] * weight
    blended = blended + tracers[:, 0:LEAF].astype(F32) * kept

    lower = jnp.concatenate([rest, blended, jnp.zeros((BACK - REST, LEAF), F32)], axis=0)
    message = dot(place[...], lower.astype(BF), 1, 1)
    back[...] = message.reshape(DEV, CAP, BACK).astype(BF)

    def send_back(j, carry):
        there = lax.rem(me + j, DEV)
        remote(back.at[there], arrived_back.at[me], move_send.at[1], move_recv.at[1], there).start()
        return carry

    lax.fori_loop(1, DEV, send_back, 0)
    arrived_front[pl.ds(me, 1)] = front[pl.ds(me, 1)]
    arrived_back[pl.ds(me, 1)] = back[pl.ds(me, 1)]

    for copy in halos:
        copy.wait_send()
    all_poles.wait_send()
    pair.wait_send()
    to_holder.wait_send()
    to_pair.wait_send()
    most = pl.ds(0, DEV - 1)
    for k, (sent, got) in enumerate(((front, arrived_front), (back, arrived_back))):
        last = remote(sent.at[most], got.at[most], move_send.at[k], move_recv.at[k], partner)
        last.wait_send()
        last.wait_recv()


def step(*args):
    (
        coeffs,
        tracer,
        up_op,
        far_ops,
        down_op,
        near_ops,
        face_dirs,
        leaf_octant,
        far_src,
        far_type,
        near_list,
        near_type,
        new_owner,
    ) = args
    whole = pl.BlockSpec(memory_space=VMEM)
    anywhere = pl.BlockSpec(memory_space=pl.ANY)
    dma = pltpu.SemaphoreType.DMA
    return pl.pallas_call(
        step_kernel,
        name="step",
        out_shape=(
            jax.ShapeDtypeStruct((DEV, CAP, FRONT), BF),
            jax.ShapeDtypeStruct((DEV, CAP, BACK), BF),
        ),
        in_specs=[anywhere] * 6 + [pl.BlockSpec(memory_space=pltpu.SMEM)] + [anywhere] * 6,
        out_specs=(whole, whole),
        scratch_shapes=[
            VMEM((COEF, 2 * LEAF), BF),
            VMEM((NCOEF, 2 * LEAF), BF),
            VMEM((MULT, COEF), BF),
            VMEM((MULT * FTYPES, MULT), BF),
            VMEM((MULT, COEF), BF),
            VMEM((1, LEAF), I32),
            VMEM((OCT_DEV, FAR_K), I32),
            VMEM((OCT_DEV, FAR_K), I32),
            VMEM((NEAR_K, LEAF), I32),
            VMEM((NEAR_K, LEAF), I32),
            VMEM((1, LEAF), I32),
            VMEM((NBLK * 256, COEF), BF),
            VMEM((NBLK * OBLK, NTYPES * KPAD), BF),
            VMEM((NTYPES, 2 * LEAF, LEAF), BF),
            VMEM((NTYPES * KPAD, LEAF), BF),
            VMEM((NTYPES, NCOEF, LEAF), F32),
            VMEM((DEV, 16, 256), BF),
            VMEM((128, OCTANTS), BF),
            VMEM((16, 256), BF),
            VMEM((16, 256), BF),
            VMEM((16, 256), BF),
            VMEM((DEV * CAP, LEAF), BF),
            VMEM((FRONT, LEAF), F32),
            VMEM((DEV, CAP, FRONT), BF),
            VMEM((DEV, CAP, BACK), BF),
            VMEM((3, NEAR_K, LEAF), I32),
            dma((12,)),
            dma((4,)),
            dma((4,)),
            dma,
            dma,
            dma,
            dma,
            dma((2,)),
            dma((2,)),
            dma((2,)),
            dma((2,)),
        ],
        compiler_params=pltpu.CompilerParams(
            collective_id=0, has_side_effects=True, vmem_limit_bytes=67_043_328
        ),
    )(
        coeffs,
        tracer,
        up_op,
        far_ops.reshape(MULT * FTYPES, MULT),
        down_op.T,
        near_ops.reshape(COEF * NTYPES, COEF),
        face_dirs,
        leaf_octant.reshape(1, LEAF),
        far_src.T,
        far_type.T,
        near_list,
        near_type,
        new_owner.reshape(1, LEAF),
    )


def turn_kernel(front, back, moved):
    slots = DEV * CAP
    moved[0:FRONT, :] = front[...].astype(F32).reshape(slots, FRONT).T.astype(BF)
    turned = back[...].astype(F32).reshape(slots, BACK).T
    moved[FRONT : COEF + NCOEF, :] = turned[0:REST].astype(BF)


def local(*args):
    return pl.pallas_call(
        turn_kernel,
        name="turn",
        out_shape=jax.ShapeDtypeStruct((COEF + NCOEF, DEV * CAP), BF),
    )(*step(*args))


def solution(mesh):
    split = P(None, GRP_SEG)
    in_specs = (
        split,
        split,
        P(),
        P(),
        P(),
        P(),
        P(),
        P(GRP_SEG),
        split,
        split,
        split,
        split,
        P(GRP_SEG, None),
    )
    return jax.shard_map(local, mesh=mesh, in_specs=in_specs, out_specs=split, check_vma=False)
```

```python
import functools

import jax
import jax.numpy as jnp
from jax import lax
from jax.experimental import pallas as pl
from jax.experimental.pallas import tpu as pltpu
from jax.sharding import PartitionSpec as P

NCOEF = 286
COEF = 858
MULT = 168
NTYPES = 8
NEAR_K = 27
FTYPES = 16
FAR_K = 189
LEAF = 256
HALO = 128
OCT_DEV = 8
OCTANTS = 1024
CAP = 4
SEG = 64
DEV = 128
KPAD = 896
OBLK = 32
NBLK = 27
FRONT = 640
BACK = 512
REST = 504
LINE = 4
PLANE = 16
TARGETS = 144
CUT = 88
CHUNKS = 9
CHUNK = 768
CUT_BACK = 80
GREETINGS = 22
GRP_SEG = ("grp", "seg")
LOGICAL = pl.DeviceIdType.LOGICAL
BF = jnp.bfloat16
F32 = jnp.float32
I32 = jnp.int32
VMEM = pltpu.VMEM


def dot(a, b, ca=1, cb=0):
    return lax.dot_general(a, b, (((ca,), (cb,)), ((), ())), preferred_element_type=F32)


def hot(mask):
    return jnp.where(mask, 1.0, 0.0).astype(BF)


def iota(shape, dim):
    return lax.broadcasted_iota(I32, shape, dim)


def remote(src, dst, send_sem, recv_sem, device):
    return pltpu.make_async_remote_copy(
        src_ref=src,
        dst_ref=dst,
        send_sem=send_sem,
        recv_sem=recv_sem,
        device_id=device,
        device_id_type=LOGICAL,
    )


def step_kernel(
    coeffs_hbm,
    tracer_hbm,
    up_hbm,
    far_hbm,
    down_hbm,
    near_hbm,
    face_dirs,
    octant_hbm,
    source_hbm,
    type_hbm,
    list_hbm,
    kind_hbm,
    owner_hbm,
    arrived_front,
    arrived_back,
    window,
    tracers,
    up_op,
    far_ops,
    down_op,
    leaf_octant,
    far_src,
    far_type,
    near_list,
    near_type,
    new_owner,
    raw_ops,
    ops,
    counts,
    group,
    mixed,
    poles,
    far_count,
    source_in,
    type_in,
    source_edge,
    type_edge,
    place,
    velocity,
    front,
    back,
    slots,
    load_sem,
    halo_send,
    halo_recv,
    list_send,
    list_recv,
    line_send,
    line_recv,
    plane_send,
    plane_recv,
    pair_send,
    pair_recv,
    move_send,
    move_recv,
):
    grp = lax.axis_index("grp")
    seg = lax.axis_index("seg")
    me = grp * SEG + seg
    partner = (1 - grp) * SEG + seg
    own_lanes = pl.ds(0, LEAF)
    rows = COEF * NTYPES

    def load(source, target, k):
        copy = pltpu.make_async_copy(source, target, load_sem.at[k])
        copy.start()
        return copy

    loads = [
        load(coeffs_hbm, window.at[:, own_lanes], 0),
        load(up_hbm, up_op, 1),
        load(octant_hbm, leaf_octant, 2),
        load(tracer_hbm, tracers.at[:, own_lanes], 3),
        load(source_hbm, far_src, 4),
        load(type_hbm, far_type, 5),
        load(list_hbm, near_list, 6),
        load(kind_hbm, near_type, 7),
        load(owner_hbm, new_owner, 8),
        load(far_hbm, far_ops, 9),
        load(down_hbm, down_op, 10),
    ]
    chunks = []
    for k in range(CHUNKS):
        start = k * CHUNK
        part_of = pl.ds(start, min(CHUNK, rows - start))
        chunks.append(load(near_hbm.at[part_of], raw_ops.at[part_of], 11 + k))

    right = grp * SEG + lax.rem(seg + 1, SEG)
    left = grp * SEG + lax.rem(seg + SEG - 1, SEG)
    holder = jnp.where(lax.rem(me, 2) == 0, me + 1, lax.rem(me + SEG + 1, DEV))
    lister = jnp.where(lax.rem(me, 2) == 0, lax.rem(me + SEG - 1, DEV), me - 1)

    def on_line(j):
        return grp * SEG + (seg // LINE) * LINE + lax.rem(seg + j, LINE)

    def in_plane(j):
        return grp * SEG + lax.rem(seg + LINE * j, SEG)

    barrier = pltpu.get_barrier_semaphore()

    def greet(there):
        pl.semaphore_signal(barrier, inc=1, device_id=there, device_id_type=LOGICAL)

    greet(right)
    greet(left)
    for j in range(1, LINE):
        greet(on_line(j))
    greet(partner)
    greet(lister)

    def greet_plane(j, carry):
        greet(in_plane(j))
        return carry

    lax.fori_loop(1, PLANE, greet_plane, 0)

    for copy in loads[0:3]:
        copy.wait()
    leaf_pole = dot(up_op[...], window[:, 0:LEAF]).astype(BF)
    piece = hot(iota((16, LEAF), 0) == leaf_octant[...] - me * OCT_DEV)
    part = dot(piece, leaf_pole, 1, 1)
    ninth = part[8:9, :]
    part_row = iota((8, MULT), 0)
    lane_in = iota((MULT, 256), 0)
    lane_out = iota((MULT, 256), 1)
    spread = (
        (part[0:8, :], lane_out == lane_in),
        (jnp.where(part_row == 0, ninth, 0.0), (lane_out == lane_in + MULT) & (lane_in < CUT)),
        (jnp.where(part_row == 1, ninth, 0.0), (lane_out == lane_in + CUT_BACK) & (lane_in >= CUT)),
    )
    packed = jnp.zeros((8, 256), F32)
    for value, lanes in spread:
        packed = packed + dot(value.astype(BF), hot(lanes))
    poles[pl.ds(me, 1)] = packed.astype(BF)[None]

    for copy in loads[3:6]:
        copy.wait()
    pl.semaphore_wait(barrier, GREETINGS)
    for j in range(1, LINE):
        remote(poles.at[me], poles.at[me], line_send, line_recv, on_line(j)).start()
    low = pl.ds(0, HALO)
    high = pl.ds(HALO, HALO)
    to_low = pl.ds(LEAF, HALO)
    to_high = pl.ds(LEAF + HALO, HALO)
    halos = [
        remote(src.at[:, lanes], src.at[:, there], halo_send.at[k], halo_recv.at[k], device)
        for k, (src, lanes, there, device) in enumerate(
            (
                (window, high, to_low, right),
                (window, low, to_high, left),
                (tracers, high, to_low, right),
                (tracers, low, to_high, left),
            )
        )
    ]
    lists = [
        remote(src, there, list_send.at[k], list_recv.at[k], device)
        for k, (src, there, device) in enumerate(
            (
                (far_src, source_in, holder),
                (far_type, type_in, holder),
                (far_src, source_edge, partner),
                (far_type, type_edge, partner),
            )
        )
    ]
    for copy in halos + lists:
        copy.start()

    for copy in loads[6:9]:
        copy.wait()
    listed = near_list[...]
    inside = (listed >= HALO) & (listed < HALO + LEAF)
    spot = jnp.where(inside, listed - HALO, jnp.where(listed < HALO, listed + LEAF, listed))
    kind = near_type[...]
    one = jnp.ones_like(kind)
    first_word = jnp.where(kind < 4, one << (8 * jnp.minimum(kind, 3)), 0)
    other_word = jnp.where(
        (kind >= 4) & (kind < NTYPES), one << (8 * (jnp.clip(kind, 4, 7) - 4)), 0
    )
    slots[0] = spot
    slots[1] = first_word
    slots[2] = other_word

    def count_rows(block, carry):
        base = pl.multiple_of(block * 32, 32)
        place_of = iota((32, LEAF), 0) + base
        first = jnp.zeros((32, LEAF), I32)
        other = jnp.zeros((32, LEAF), I32)
        for k in range(NEAR_K):
            here = place_of == slots[0, k : k + 1, :]
            first = first + jnp.where(here, slots[1, k : k + 1, :], 0)
            other = other + jnp.where(here, slots[2, k : k + 1, :], 0)
        for t in range(NTYPES):
            word = first if t < 4 else other
            value = lax.shift_right_logical(word, jnp.full_like(word, 8 * (t % 4))) & 255
            lanes = slice((t % 2) * LEAF, (t % 2 + 1) * LEAF)
            counts[t // 2, pl.ds(base, 32), lanes] = value.astype(F32).astype(BF)
        return carry

    lax.fori_loop(0, 16, count_rows, 0)

    all_line = remote(
        poles.at[pl.ds(0, LINE - 1)], poles.at[pl.ds(0, LINE - 1)], line_send, line_recv, partner
    )
    all_line.wait_recv()
    line = poles.at[pl.ds(grp * SEG + (seg // LINE) * LINE, LINE)]

    def send_line(j, carry):
        remote(line, line, plane_send, plane_recv, in_plane(j)).start()
        return carry

    lax.fori_loop(1, PLANE, send_line, 0)

    owner_row = new_owner[...].astype(F32)
    leaf_row = iota((LEAF, LEAF), 0)
    leaf_col = iota((LEAF, LEAF), 1)
    owner = jnp.sum(jnp.where(leaf_row == leaf_col, owner_row, 0.0), axis=1, keepdims=True)
    before = (leaf_row < leaf_col) & (owner == owner_row)
    rank = jnp.sum(jnp.where(before, 1.0, 0.0), axis=0, keepdims=True)
    target = (owner_row * float(CAP) + rank).astype(I32)
    place[...] = hot(iota((DEV * CAP, LEAF), 0) == target)

    for copy in lists:
        copy.wait_recv()
    even = lax.rem(jnp.full((1, FAR_K), me, I32), 2) == 0
    lane = iota((FTYPES, OCTANTS), 1)
    for c in range(9):
        if c < OCT_DEV:
            source, kind_row = source_in[c : c + 1, :], type_in[c : c + 1, :]
        else:
            source = jnp.where(even, far_src[0:1, :], source_edge[0:1, :])
            kind_row = jnp.where(even, far_type[0:1, :], type_edge[0:1, :])
        source_hot = hot(iota((OCTANTS, FAR_K), 0) == source)
        kind_hot = hot(iota((FTYPES, FAR_K), 0) == kind_row)
        number = dot(kind_hot, source_hot, 1, 1)
        first = jnp.where(lax.rem(lane, 8) == 0, pltpu.roll(number, OCTANTS - 8, 1), 0.0)
        second = jnp.where(lax.rem(lane, 8) == 1, pltpu.roll(number, OCTANTS - 7, 1), 0.0)
        for k, value in enumerate((number, first, second)):
            at = k * TARGETS + c * FTYPES
            far_count[at : at + FTYPES, :] = value.astype(BF)

    raw_ops[rows : NBLK * 256, :] = jnp.zeros((NBLK * 256 - rows, COEF), BF)
    for t in range(NTYPES):
        ops[:, t * KPAD + 768 : (t + 1) * KPAD] = jnp.zeros((NBLK * OBLK, 128), BF)
        group[t * KPAD + 848 : (t + 1) * KPAD, :] = jnp.zeros((48, LEAF), BF)
    turn_row = iota((256, 256), 0)
    turn = hot(iota((256, 256), 1) == lax.rem(turn_row, OBLK) * NTYPES + turn_row // OBLK)
    for copy in loads[9:11]:
        copy.wait()

    def turn_blocks(b, carry):
        for part in range(3):
            at = b * 3 + part
            block = raw_ops[pl.ds(pl.multiple_of(at * 256, 256), 256), :]
            turned = dot(turn, block).astype(BF)
            out_rows = pl.ds(pl.multiple_of(at * OBLK, OBLK), OBLK)
            for t in range(NTYPES):
                ops[out_rows, t * KPAD : t * KPAD + COEF] = turned[t * OBLK : (t + 1) * OBLK, :]
        return carry

    for k, copy in enumerate(chunks):
        copy.wait()
        turn_blocks(k, 0)

    rest_of = pl.ds(0, SEG - LINE)
    all_plane = remote(poles.at[rest_of], poles.at[rest_of], plane_send, plane_recv, partner)
    all_plane.wait_recv()
    mine = poles.at[pl.ds(grp * SEG, SEG)]
    pair = remote(mine, mine, pair_send, pair_recv, partner)
    pair.start()

    for copy in halos:
        copy.wait_recv()

    def gather_kinds(two, carry):
        base = two * 2 * KPAD
        total = dot(window[...], counts[two]).astype(BF)
        group[pl.ds(base, COEF), :] = total[:, 0:LEAF]
        group[pl.ds(base + KPAD, COEF), :] = total[:, LEAF : 2 * LEAF]
        blend = dot(tracers[...], counts[two])
        mixed[two * 2, 0:NCOEF, :] = blend[:, 0:LEAF]
        mixed[two * 2 + 1, 0:NCOEF, :] = blend[:, LEAF : 2 * LEAF]
        return carry

    for two in range(NTYPES // 2):
        gather_kinds(two, 0)

    def near_rows(block, carry):
        here = pl.ds(pl.multiple_of(block * 320, 32), 320)
        velocity[here, :] = dot(ops[here, :], group[...])
        return carry

    lax.fori_loop(0, 2, near_rows, 0)

    pair.wait_recv()
    every = poles[...].astype(F32).reshape(OCTANTS, 256).astype(BF)
    sums = dot(far_count[...], every)
    lane = iota((TARGETS, 256), 1)
    first = pltpu.roll(sums[TARGETS : 2 * TARGETS], 256 - MULT, 1)
    second = pltpu.roll(sums[2 * TARGETS : 3 * TARGETS], 256 - CUT_BACK, 1)
    extra = jnp.where(lane < CUT, first, jnp.where(lane < MULT, second, 0.0))
    grouped = (sums[0:TARGETS] + extra).astype(BF)[:, 0:MULT]
    shifted = dot(far_ops[...], grouped, 1, 1)
    far_row = iota((MULT * FTYPES, TARGETS), 0)
    same = lax.rem(iota((MULT * FTYPES, TARGETS), 1), FTYPES) == lax.rem(far_row, FTYPES)
    shifted = jnp.where(same, shifted, 0.0).astype(BF)
    kinds = hot(iota((MULT, MULT * FTYPES), 1) // FTYPES == iota((MULT, MULT * FTYPES), 0))
    by_kind = dot(kinds, shifted).astype(BF)
    fold = hot(iota((16, TARGETS), 1) // FTYPES == iota((16, TARGETS), 0))
    nine = dot(fold, by_kind, 1, 1).astype(BF)
    leaf_local = dot(nine, piece, 0, 0).astype(BF)
    velocity[...] = velocity[...] + dot(down_op[:, 0:FRONT], leaf_local, 0, 0)

    message = dot(place[...], velocity[0:FRONT, :].astype(BF), 1, 1)
    front[...] = message.reshape(DEV, CAP, FRONT).astype(BF)

    def send_front(j, carry):
        there = lax.rem(me + j, DEV)
        remote(front.at[there], arrived_front.at[me], move_send.at[0], move_recv.at[0], there).start()
        return carry

    lax.fori_loop(1, DEV, send_front, 0)

    rest = dot(ops[FRONT : NBLK * OBLK, :], group[...])[0 : COEF - FRONT, :]
    rest = rest + dot(down_op[:, FRONT:COEF], leaf_local, 0, 0)

    flows = []
    total_in = jnp.zeros((1, LEAF), F32)
    for t in range(NTYPES):
        normal = (
            face_dirs[0, t] * velocity[0:1, :]
            + face_dirs[1, t] * velocity[NCOEF : NCOEF + 1, :]
            + face_dirs[2, t] * velocity[2 * NCOEF : 2 * NCOEF + 1, :]
        )
        number = jnp.sum(jnp.where(kind == t, 1.0, 0.0), axis=0, keepdims=True)
        flow = jnp.maximum(normal, 0.0)
        flows.append((flow, number))
        total_in = total_in + flow * number
    denominator = 1.0 + total_in
    kept = jnp.ones((1, LEAF), F32)
    blended = jnp.zeros((NCOEF, LEAF), F32)
    for t, (flow, number) in enumerate(flows):
        weight = flow / denominator
        kept = kept - weight * number
        blended = blended + mixed[t, 0:NCOEF, :] * weight
    blended = blended + tracers[:, 0:LEAF].astype(F32) * kept

    lower = jnp.concatenate([rest, blended, jnp.zeros((BACK - REST, LEAF), F32)], axis=0)
    message = dot(place[...], lower.astype(BF), 1, 1)
    back[...] = message.reshape(DEV, CAP, BACK).astype(BF)

    def send_back(j, carry):
        there = lax.rem(me + j, DEV)
        remote(back.at[there], arrived_back.at[me], move_send.at[1], move_recv.at[1], there).start()
        return carry

    lax.fori_loop(1, DEV, send_back, 0)
    arrived_front[pl.ds(me, 1)] = front[pl.ds(me, 1)]
    arrived_back[pl.ds(me, 1)] = back[pl.ds(me, 1)]

    for copy in halos + lists:
        copy.wait_send()
    all_line.wait_send()
    all_plane.wait_send()
    pair.wait_send()
    most = pl.ds(0, DEV - 1)
    for k, (sent, got) in enumerate(((front, arrived_front), (back, arrived_back))):
        last = remote(sent.at[most], got.at[most], move_send.at[k], move_recv.at[k], partner)
        last.wait_send()
        last.wait_recv()


def step(*args):
    (
        coeffs,
        tracer,
        up_op,
        far_ops,
        down_op,
        near_ops,
        face_dirs,
        leaf_octant,
        far_src,
        far_type,
        near_list,
        near_type,
        new_owner,
    ) = args
    whole = pl.BlockSpec(memory_space=VMEM)
    anywhere = pl.BlockSpec(memory_space=pl.ANY)
    dma = pltpu.SemaphoreType.DMA
    return pl.pallas_call(
        step_kernel,
        name="step",
        out_shape=(
            jax.ShapeDtypeStruct((DEV, CAP, FRONT), BF),
            jax.ShapeDtypeStruct((DEV, CAP, BACK), BF),
        ),
        in_specs=[anywhere] * 6 + [pl.BlockSpec(memory_space=pltpu.SMEM)] + [anywhere] * 6,
        out_specs=(whole, whole),
        scratch_shapes=[
            VMEM((COEF, 2 * LEAF), BF),
            VMEM((NCOEF, 2 * LEAF), BF),
            VMEM((MULT, COEF), BF),
            VMEM((MULT * FTYPES, MULT), BF),
            VMEM((MULT, COEF), BF),
            VMEM((1, LEAF), I32),
            VMEM((OCT_DEV, FAR_K), I32),
            VMEM((OCT_DEV, FAR_K), I32),
            VMEM((NEAR_K, LEAF), I32),
            VMEM((NEAR_K, LEAF), I32),
            VMEM((1, LEAF), I32),
            VMEM((NBLK * 256, COEF), BF),
            VMEM((NBLK * OBLK, NTYPES * KPAD), BF),
            VMEM((NTYPES // 2, 2 * LEAF, 2 * LEAF), BF),
            VMEM((NTYPES * KPAD, LEAF), BF),
            VMEM((NTYPES, 288, LEAF), F32),
            VMEM((DEV, 8, 256), BF),
            VMEM((3 * TARGETS, OCTANTS), BF),
            VMEM((OCT_DEV, FAR_K), I32),
            VMEM((OCT_DEV, FAR_K), I32),
            VMEM((OCT_DEV, FAR_K), I32),
            VMEM((OCT_DEV, FAR_K), I32),
            VMEM((DEV * CAP, LEAF), BF),
            VMEM((FRONT, LEAF), F32),
            VMEM((DEV, CAP, FRONT), BF),
            VMEM((DEV, CAP, BACK), BF),
            VMEM((3, NEAR_K, LEAF), I32),
            dma((11 + CHUNKS,)),
            dma((4,)),
            dma((4,)),
            dma((4,)),
            dma((4,)),
            dma,
            dma,
            dma,
            dma,
            dma,
            dma,
            dma((2,)),
            dma((2,)),
        ],
        compiler_params=pltpu.CompilerParams(
            collective_id=0, has_side_effects=True, vmem_limit_bytes=67_043_328
        ),
    )(
        coeffs,
        tracer,
        up_op,
        far_ops.reshape(MULT * FTYPES, MULT),
        down_op.T,
        near_ops.reshape(COEF * NTYPES, COEF),
        face_dirs,
        leaf_octant.reshape(1, LEAF),
        far_src.T,
        far_type.T,
        near_list,
        near_type,
        new_owner.reshape(1, LEAF),
    )


def turn_kernel(front, back, moved):
    slots = DEV * CAP
    moved[0:FRONT, :] = front[...].astype(F32).reshape(slots, FRONT).T.astype(BF)
    turned = back[...].astype(F32).reshape(slots, BACK).T
    moved[FRONT : COEF + NCOEF, :] = turned[0:REST].astype(BF)


def local(*args):
    return pl.pallas_call(
        turn_kernel,
        name="turn",
        out_shape=jax.ShapeDtypeStruct((COEF + NCOEF, DEV * CAP), BF),
    )(*step(*args))


def solution(mesh):
    split = P(None, GRP_SEG)
    in_specs = (
        split,
        split,
        P(),
        P(),
        P(),
        P(),
        P(),
        P(GRP_SEG),
        split,
        split,
        split,
        split,
        P(GRP_SEG, None),
    )
    return jax.shard_map(local, mesh=mesh, in_specs=in_specs, out_specs=split, check_vma=False)
```

```python
import functools

import jax
import jax.numpy as jnp
from jax import lax
from jax.experimental import pallas as pl
from jax.experimental.pallas import tpu as pltpu
from jax.sharding import PartitionSpec as P

NCOEF = 286
COEF = 858
MULT = 168
NTYPES = 8
NEAR_K = 27
FTYPES = 16
FAR_K = 189
LEAF = 256
HALO = 128
OCT_DEV = 8
OCTANTS = 1024
CAP = 4
SEG = 64
DEV = 128
KPAD = 896
OBLK = 32
NBLK = 27
PART = 384
PARTS = 3
REST = 376
LINE = 4
PLANE = 16
TARGETS = 144
CUT = 88
CHUNKS = 9
CHUNK = 768
CUT_BACK = 80
GREETINGS = 22
GRP_SEG = ("grp", "seg")
LOGICAL = pl.DeviceIdType.LOGICAL
BF = jnp.bfloat16
F32 = jnp.float32
I32 = jnp.int32
VMEM = pltpu.VMEM


def dot(a, b, ca=1, cb=0):
    return lax.dot_general(a, b, (((ca,), (cb,)), ((), ())), preferred_element_type=F32)


def hot(mask):
    return jnp.where(mask, 1.0, 0.0).astype(BF)


def iota(shape, dim):
    return lax.broadcasted_iota(I32, shape, dim)


def remote(src, dst, send_sem, recv_sem, device):
    return pltpu.make_async_remote_copy(
        src_ref=src,
        dst_ref=dst,
        send_sem=send_sem,
        recv_sem=recv_sem,
        device_id=device,
        device_id_type=LOGICAL,
    )


def step_kernel(
    coeffs_hbm,
    tracer_hbm,
    up_hbm,
    far_hbm,
    down_hbm,
    near_hbm,
    face_dirs,
    octant_hbm,
    source_hbm,
    type_hbm,
    list_hbm,
    kind_hbm,
    owner_hbm,
    arrived_0,
    arrived_1,
    arrived_2,
    window,
    tracers,
    up_op,
    far_ops,
    down_op,
    leaf_octant,
    far_src,
    far_type,
    near_list,
    near_type,
    new_owner,
    raw_ops,
    ops,
    counts,
    group,
    mixed,
    poles,
    far_count,
    source_in,
    type_in,
    source_edge,
    type_edge,
    place,
    velocity,
    leaving,
    slots,
    load_sem,
    halo_send,
    halo_recv,
    list_send,
    list_recv,
    keep_sem,
    line_send,
    line_recv,
    plane_send,
    plane_recv,
    pair_send,
    pair_recv,
    move_send,
    move_recv,
):
    grp = lax.axis_index("grp")
    seg = lax.axis_index("seg")
    me = grp * SEG + seg
    partner = (1 - grp) * SEG + seg
    own_lanes = pl.ds(0, LEAF)
    rows = COEF * NTYPES

    def load(source, target, k):
        copy = pltpu.make_async_copy(source, target, load_sem.at[k])
        copy.start()
        return copy

    loads = [
        load(coeffs_hbm, window.at[:, own_lanes], 0),
        load(up_hbm, up_op, 1),
        load(octant_hbm, leaf_octant, 2),
        load(tracer_hbm, tracers.at[:, own_lanes], 3),
        load(source_hbm, far_src, 4),
        load(type_hbm, far_type, 5),
        load(list_hbm, near_list, 6),
        load(kind_hbm, near_type, 7),
        load(owner_hbm, new_owner, 8),
        load(far_hbm, far_ops, 9),
        load(down_hbm, down_op, 10),
    ]
    chunks = []
    for k in range(CHUNKS):
        start = k * CHUNK
        part_of = pl.ds(start, min(CHUNK, rows - start))
        chunks.append(load(near_hbm.at[part_of], raw_ops.at[part_of], 11 + k))

    right = grp * SEG + lax.rem(seg + 1, SEG)
    left = grp * SEG + lax.rem(seg + SEG - 1, SEG)
    holder = jnp.where(lax.rem(me, 2) == 0, me + 1, lax.rem(me + SEG + 1, DEV))
    lister = jnp.where(lax.rem(me, 2) == 0, lax.rem(me + SEG - 1, DEV), me - 1)

    def on_line(j):
        return grp * SEG + (seg // LINE) * LINE + lax.rem(seg + j, LINE)

    def in_plane(j):
        return grp * SEG + lax.rem(seg + LINE * j, SEG)

    barrier = pltpu.get_barrier_semaphore()

    def greet(there):
        pl.semaphore_signal(barrier, inc=1, device_id=there, device_id_type=LOGICAL)

    greet(right)
    greet(left)
    for j in range(1, LINE):
        greet(on_line(j))
    greet(partner)
    greet(lister)

    def greet_plane(j, carry):
        greet(in_plane(j))
        return carry

    lax.fori_loop(1, PLANE, greet_plane, 0)

    for copy in loads[0:3]:
        copy.wait()
    leaf_pole = dot(up_op[...], window[:, 0:LEAF]).astype(BF)
    piece = hot(iota((16, LEAF), 0) == leaf_octant[...] - me * OCT_DEV)
    part = dot(piece, leaf_pole, 1, 1)
    ninth = part[8:9, :]
    part_row = iota((8, MULT), 0)
    lane_in = iota((MULT, 256), 0)
    lane_out = iota((MULT, 256), 1)
    spread = (
        (part[0:8, :], lane_out == lane_in),
        (jnp.where(part_row == 0, ninth, 0.0), (lane_out == lane_in + MULT) & (lane_in < CUT)),
        (jnp.where(part_row == 1, ninth, 0.0), (lane_out == lane_in + CUT_BACK) & (lane_in >= CUT)),
    )
    packed = jnp.zeros((8, 256), F32)
    for value, lanes in spread:
        packed = packed + dot(value.astype(BF), hot(lanes))
    poles[pl.ds(me, 1)] = packed.astype(BF)[None]

    for copy in loads[3:6]:
        copy.wait()
    pl.semaphore_wait(barrier, GREETINGS)
    for j in range(1, LINE):
        remote(poles.at[me], poles.at[me], line_send, line_recv, on_line(j)).start()
    low = pl.ds(0, HALO)
    high = pl.ds(HALO, HALO)
    to_low = pl.ds(LEAF, HALO)
    to_high = pl.ds(LEAF + HALO, HALO)
    halos = [
        remote(src.at[:, lanes], src.at[:, there], halo_send.at[k], halo_recv.at[k], device)
        for k, (src, lanes, there, device) in enumerate(
            (
                (window, high, to_low, right),
                (window, low, to_high, left),
                (tracers, high, to_low, right),
                (tracers, low, to_high, left),
            )
        )
    ]
    lists = [
        remote(src, there, list_send.at[k], list_recv.at[k], device)
        for k, (src, there, device) in enumerate(
            (
                (far_src, source_in, holder),
                (far_type, type_in, holder),
                (far_src, source_edge, partner),
                (far_type, type_edge, partner),
            )
        )
    ]
    for copy in halos + lists:
        copy.start()

    for copy in loads[6:9]:
        copy.wait()
    listed = near_list[...]
    inside = (listed >= HALO) & (listed < HALO + LEAF)
    spot = jnp.where(inside, listed - HALO, jnp.where(listed < HALO, listed + LEAF, listed))
    kind = near_type[...]
    one = jnp.ones_like(kind)
    first_word = jnp.where(kind < 4, one << (8 * jnp.minimum(kind, 3)), 0)
    other_word = jnp.where(
        (kind >= 4) & (kind < NTYPES), one << (8 * (jnp.clip(kind, 4, 7) - 4)), 0
    )
    slots[0] = spot
    slots[1] = first_word
    slots[2] = other_word

    def count_rows(block, carry):
        base = pl.multiple_of(block * 32, 32)
        place_of = iota((32, LEAF), 0) + base
        first = jnp.zeros((32, LEAF), I32)
        other = jnp.zeros((32, LEAF), I32)
        for k in range(NEAR_K):
            here = place_of == slots[0, k : k + 1, :]
            first = first + jnp.where(here, slots[1, k : k + 1, :], 0)
            other = other + jnp.where(here, slots[2, k : k + 1, :], 0)
        for t in range(NTYPES):
            word = first if t < 4 else other
            value = lax.shift_right_logical(word, jnp.full_like(word, 8 * (t % 4))) & 255
            lanes = slice((t % 2) * LEAF, (t % 2 + 1) * LEAF)
            counts[t // 2, pl.ds(base, 32), lanes] = value.astype(F32).astype(BF)
        return carry

    lax.fori_loop(0, 16, count_rows, 0)

    all_line = remote(
        poles.at[pl.ds(0, LINE - 1)], poles.at[pl.ds(0, LINE - 1)], line_send, line_recv, partner
    )
    all_line.wait_recv()
    line = poles.at[pl.ds(grp * SEG + (seg // LINE) * LINE, LINE)]

    def send_line(j, carry):
        remote(line, line, plane_send, plane_recv, in_plane(j)).start()
        return carry

    lax.fori_loop(1, PLANE, send_line, 0)

    owner_row = new_owner[...].astype(F32)
    leaf_row = iota((LEAF, LEAF), 0)
    leaf_col = iota((LEAF, LEAF), 1)
    owner = jnp.sum(jnp.where(leaf_row == leaf_col, owner_row, 0.0), axis=1, keepdims=True)
    before = (leaf_row < leaf_col) & (owner == owner_row)
    rank = jnp.sum(jnp.where(before, 1.0, 0.0), axis=0, keepdims=True)
    target = (owner_row * float(CAP) + rank).astype(I32)
    place[...] = hot(iota((DEV * CAP, LEAF), 0) == target)

    for copy in lists:
        copy.wait_recv()
    even = lax.rem(jnp.full((1, FAR_K), me, I32), 2) == 0
    lane = iota((FTYPES, OCTANTS), 1)
    for c in range(9):
        if c < OCT_DEV:
            source, kind_row = source_in[c : c + 1, :], type_in[c : c + 1, :]
        else:
            source = jnp.where(even, far_src[0:1, :], source_edge[0:1, :])
            kind_row = jnp.where(even, far_type[0:1, :], type_edge[0:1, :])
        source_hot = hot(iota((OCTANTS, FAR_K), 0) == source)
        kind_hot = hot(iota((FTYPES, FAR_K), 0) == kind_row)
        number = dot(kind_hot, source_hot, 1, 1)
        first = jnp.where(lax.rem(lane, 8) == 0, pltpu.roll(number, OCTANTS - 8, 1), 0.0)
        second = jnp.where(lax.rem(lane, 8) == 1, pltpu.roll(number, OCTANTS - 7, 1), 0.0)
        for k, value in enumerate((number, first, second)):
            at = k * TARGETS + c * FTYPES
            far_count[at : at + FTYPES, :] = value.astype(BF)

    raw_ops[rows : NBLK * 256, :] = jnp.zeros((NBLK * 256 - rows, COEF), BF)
    for t in range(NTYPES):
        ops[:, t * KPAD + 768 : (t + 1) * KPAD] = jnp.zeros((NBLK * OBLK, 128), BF)
        group[t * KPAD + 848 : (t + 1) * KPAD, :] = jnp.zeros((48, LEAF), BF)
    turn_row = iota((256, 256), 0)
    turn = hot(iota((256, 256), 1) == lax.rem(turn_row, OBLK) * NTYPES + turn_row // OBLK)
    for copy in loads[9:11]:
        copy.wait()

    def turn_blocks(b, carry):
        for part in range(3):
            at = b * 3 + part
            block = raw_ops[pl.ds(pl.multiple_of(at * 256, 256), 256), :]
            turned = dot(turn, block).astype(BF)
            out_rows = pl.ds(pl.multiple_of(at * OBLK, OBLK), OBLK)
            for t in range(NTYPES):
                ops[out_rows, t * KPAD : t * KPAD + COEF] = turned[t * OBLK : (t + 1) * OBLK, :]
        return carry

    for k, copy in enumerate(chunks):
        copy.wait()
        turn_blocks(k, 0)

    rest_of = pl.ds(0, SEG - LINE)
    all_plane = remote(poles.at[rest_of], poles.at[rest_of], plane_send, plane_recv, partner)
    all_plane.wait_recv()
    mine = poles.at[pl.ds(grp * SEG, SEG)]
    pair = remote(mine, mine, pair_send, pair_recv, partner)
    pair.start()

    for copy in halos:
        copy.wait_recv()

    def gather_kinds(two, carry):
        base = two * 2 * KPAD
        total = dot(window[...], counts[two]).astype(BF)
        group[pl.ds(base, COEF), :] = total[:, 0:LEAF]
        group[pl.ds(base + KPAD, COEF), :] = total[:, LEAF : 2 * LEAF]
        blend = dot(tracers[...], counts[two])
        mixed[two * 2, 0:NCOEF, :] = blend[:, 0:LEAF]
        mixed[two * 2 + 1, 0:NCOEF, :] = blend[:, LEAF : 2 * LEAF]
        return carry

    for two in range(NTYPES // 2):
        gather_kinds(two, 0)

    velocity[0:PART, :] = dot(ops[0:PART, :], group[...])

    pair.wait_recv()
    every = poles[...].astype(F32).reshape(OCTANTS, 256).astype(BF)
    sums = dot(far_count[...], every)
    lane = iota((TARGETS, 256), 1)
    first = pltpu.roll(sums[TARGETS : 2 * TARGETS], 256 - MULT, 1)
    second = pltpu.roll(sums[2 * TARGETS : 3 * TARGETS], 256 - CUT_BACK, 1)
    extra = jnp.where(lane < CUT, first, jnp.where(lane < MULT, second, 0.0))
    grouped = (sums[0:TARGETS] + extra).astype(BF)[:, 0:MULT]
    shifted = dot(far_ops[...], grouped, 1, 1)
    far_row = iota((MULT * FTYPES, TARGETS), 0)
    same = lax.rem(iota((MULT * FTYPES, TARGETS), 1), FTYPES) == lax.rem(far_row, FTYPES)
    shifted = jnp.where(same, shifted, 0.0).astype(BF)
    kinds = hot(iota((MULT, MULT * FTYPES), 1) // FTYPES == iota((MULT, MULT * FTYPES), 0))
    by_kind = dot(kinds, shifted).astype(BF)
    fold = hot(iota((16, TARGETS), 1) // FTYPES == iota((16, TARGETS), 0))
    nine = dot(fold, by_kind, 1, 1).astype(BF)
    leaf_local = dot(nine, piece, 0, 0).astype(BF)
    velocity[0:PART, :] = velocity[0:PART, :] + dot(down_op[:, 0:PART], leaf_local, 0, 0)

    arrived = (arrived_0, arrived_1, arrived_2)
    kept_here = []

    def send_part(k, value):
        message = dot(place[...], value.astype(BF), 1, 1)
        leaving[k] = message.reshape(DEV, CAP, PART).astype(BF)

        def send_one(j, carry):
            there = lax.rem(me + j, DEV)
            here = leaving.at[k, there]
            remote(here, arrived[k].at[me], move_send.at[k], move_recv.at[k], there).start()
            return carry

        lax.fori_loop(1, DEV, send_one, 0)
        copy = pltpu.make_async_copy(leaving.at[k, me], arrived[k].at[me], keep_sem.at[k])
        copy.start()
        kept_here.append(copy)

    send_part(0, velocity[0:PART, :])
    more = dot(ops[PART : 2 * PART, :], group[...])
    velocity[PART:, :] = more + dot(down_op[:, PART : 2 * PART], leaf_local, 0, 0)
    send_part(1, velocity[PART:, :])
    rest = dot(ops[2 * PART : NBLK * OBLK, :], group[...])[0 : COEF - 2 * PART, :]
    rest = rest + dot(down_op[:, 2 * PART : COEF], leaf_local, 0, 0)

    flows = []
    total_in = jnp.zeros((1, LEAF), F32)
    for t in range(NTYPES):
        normal = (
            face_dirs[0, t] * velocity[0:1, :]
            + face_dirs[1, t] * velocity[NCOEF : NCOEF + 1, :]
            + face_dirs[2, t] * velocity[2 * NCOEF : 2 * NCOEF + 1, :]
        )
        number = jnp.sum(jnp.where(kind == t, 1.0, 0.0), axis=0, keepdims=True)
        flow = jnp.maximum(normal, 0.0)
        flows.append((flow, number))
        total_in = total_in + flow * number
    denominator = 1.0 + total_in
    kept = jnp.ones((1, LEAF), F32)
    blended = jnp.zeros((NCOEF, LEAF), F32)
    for t, (flow, number) in enumerate(flows):
        weight = flow / denominator
        kept = kept - weight * number
        blended = blended + mixed[t, 0:NCOEF, :] * weight
    blended = blended + tracers[:, 0:LEAF].astype(F32) * kept

    send_part(2, jnp.concatenate([rest, blended, jnp.zeros((PART - REST, LEAF), F32)], axis=0))

    for copy in halos + lists:
        copy.wait_send()
    all_line.wait_send()
    all_plane.wait_send()
    pair.wait_send()
    most = pl.ds(0, DEV - 1)
    for k in range(PARTS):
        kept_here[k].wait()
        sent, got = leaving.at[k, most], arrived[k].at[most]
        last = remote(sent, got, move_send.at[k], move_recv.at[k], partner)
        last.wait_send()
        last.wait_recv()


def step(*args):
    (
        coeffs,
        tracer,
        up_op,
        far_ops,
        down_op,
        near_ops,
        face_dirs,
        leaf_octant,
        far_src,
        far_type,
        near_list,
        near_type,
        new_owner,
    ) = args
    anywhere = pl.BlockSpec(memory_space=pl.ANY)
    dma = pltpu.SemaphoreType.DMA
    return pl.pallas_call(
        step_kernel,
        name="step",
        out_shape=(jax.ShapeDtypeStruct((DEV, CAP, PART), BF),) * PARTS,
        in_specs=[anywhere] * 6 + [pl.BlockSpec(memory_space=pltpu.SMEM)] + [anywhere] * 6,
        out_specs=(anywhere,) * PARTS,
        scratch_shapes=[
            VMEM((COEF, 2 * LEAF), BF),
            VMEM((NCOEF, 2 * LEAF), BF),
            VMEM((MULT, COEF), BF),
            VMEM((MULT * FTYPES, MULT), BF),
            VMEM((MULT, COEF), BF),
            VMEM((1, LEAF), I32),
            VMEM((OCT_DEV, FAR_K), I32),
            VMEM((OCT_DEV, FAR_K), I32),
            VMEM((NEAR_K, LEAF), I32),
            VMEM((NEAR_K, LEAF), I32),
            VMEM((1, LEAF), I32),
            VMEM((NBLK * 256, COEF), BF),
            VMEM((NBLK * OBLK, NTYPES * KPAD), BF),
            VMEM((NTYPES // 2, 2 * LEAF, 2 * LEAF), BF),
            VMEM((NTYPES * KPAD, LEAF), BF),
            VMEM((NTYPES, 288, LEAF), F32),
            VMEM((DEV, 8, 256), BF),
            VMEM((3 * TARGETS, OCTANTS), BF),
            VMEM((OCT_DEV, FAR_K), I32),
            VMEM((OCT_DEV, FAR_K), I32),
            VMEM((OCT_DEV, FAR_K), I32),
            VMEM((OCT_DEV, FAR_K), I32),
            VMEM((DEV * CAP, LEAF), BF),
            VMEM((2 * PART, LEAF), F32),
            VMEM((PARTS, DEV, CAP, PART), BF),
            VMEM((3, NEAR_K, LEAF), I32),
            dma((11 + CHUNKS,)),
            dma((4,)),
            dma((4,)),
            dma((4,)),
            dma((4,)),
            dma((PARTS,)),
            dma,
            dma,
            dma,
            dma,
            dma,
            dma,
            dma((PARTS,)),
            dma((PARTS,)),
        ],
        compiler_params=pltpu.CompilerParams(
            collective_id=0, has_side_effects=True, vmem_limit_bytes=67_043_328
        ),
    )(
        coeffs,
        tracer,
        up_op,
        far_ops.reshape(MULT * FTYPES, MULT),
        down_op.T,
        near_ops.reshape(COEF * NTYPES, COEF),
        face_dirs,
        leaf_octant.reshape(1, LEAF),
        far_src.T,
        far_type.T,
        near_list,
        near_type,
        new_owner.reshape(1, LEAF),
    )


def turn_kernel(first, second, third, moved, held, turned, in_sem, out_sem):
    loads = [
        pltpu.make_async_copy(source, held.at[k], in_sem.at[k])
        for k, source in enumerate((first, second, third))
    ]
    for copy in loads:
        copy.start()
    stores = []
    for k, copy in enumerate(loads):
        copy.wait()
        turned[k] = held[k].astype(F32).reshape(DEV * CAP, PART).T.astype(BF)
        count = PART if k < 2 else REST
        store = pltpu.make_async_copy(
            turned.at[k, pl.ds(0, count)], moved.at[pl.ds(k * PART, count)], out_sem.at[k]
        )
        store.start()
        stores.append(store)
    for copy in stores:
        copy.wait()


def local(*args):
    anywhere = pl.BlockSpec(memory_space=pl.ANY)
    return pl.pallas_call(
        turn_kernel,
        name="turn",
        out_shape=jax.ShapeDtypeStruct((COEF + NCOEF, DEV * CAP), BF),
        in_specs=[anywhere] * PARTS,
        out_specs=anywhere,
        scratch_shapes=[
            VMEM((PARTS, DEV, CAP, PART), BF),
            VMEM((PARTS, PART, DEV * CAP), BF),
            pltpu.SemaphoreType.DMA((PARTS,)),
            pltpu.SemaphoreType.DMA((PARTS,)),
        ],
    )(*step(*args))


def solution(mesh):
    split = P(None, GRP_SEG)
    in_specs = (
        split,
        split,
        P(),
        P(),
        P(),
        P(),
        P(),
        P(GRP_SEG),
        split,
        split,
        split,
        split,
        P(GRP_SEG, None),
    )
    return jax.shard_map(local, mesh=mesh, in_specs=in_specs, out_specs=split, check_vma=False)
```

```python
import functools

import jax
import jax.numpy as jnp
from jax import lax
from jax.experimental import pallas as pl
from jax.experimental.pallas import tpu as pltpu
from jax.sharding import PartitionSpec as P

NCOEF = 286
COEF = 858
MULT = 168
NTYPES = 8
NEAR_K = 27
FTYPES = 16
FAR_K = 189
LEAF = 256
HALO = 128
OCT_DEV = 8
OCTANTS = 1024
CAP = 4
SEG = 64
DEV = 128
KPAD = 896
OBLK = 32
NBLK = 27
FRONT = 640
BACK = 512
REST = 504
LINE = 4
PLANE = 16
TARGETS = 144
CUT = 88
CHUNKS = 9
CHUNK = 768
CUT_BACK = 80
GREETINGS = 22
GRP_SEG = ("grp", "seg")
LOGICAL = pl.DeviceIdType.LOGICAL
BF = jnp.bfloat16
F32 = jnp.float32
I32 = jnp.int32
VMEM = pltpu.VMEM


def dot(a, b, ca=1, cb=0):
    return lax.dot_general(a, b, (((ca,), (cb,)), ((), ())), preferred_element_type=F32)


def hot(mask):
    return jnp.where(mask, 1.0, 0.0).astype(BF)


def iota(shape, dim):
    return lax.broadcasted_iota(I32, shape, dim)


def remote(src, dst, send_sem, recv_sem, device):
    return pltpu.make_async_remote_copy(
        src_ref=src,
        dst_ref=dst,
        send_sem=send_sem,
        recv_sem=recv_sem,
        device_id=device,
        device_id_type=LOGICAL,
    )


def step_kernel(
    coeffs_hbm,
    tracer_hbm,
    up_hbm,
    far_hbm,
    down_hbm,
    near_hbm,
    face_dirs,
    octant_hbm,
    source_hbm,
    type_hbm,
    list_hbm,
    kind_hbm,
    owner_hbm,
    arrived_front,
    arrived_back,
    window,
    tracers,
    up_op,
    far_ops,
    down_op,
    leaf_octant,
    far_src,
    far_type,
    near_list,
    near_type,
    new_owner,
    raw_ops,
    ops,
    counts,
    group,
    mixed,
    poles,
    far_count,
    source_in,
    type_in,
    source_edge,
    type_edge,
    place,
    velocity,
    front,
    back,
    slots,
    load_sem,
    halo_send,
    halo_recv,
    list_send,
    list_recv,
    line_send,
    line_recv,
    plane_send,
    plane_recv,
    pair_send,
    pair_recv,
    move_send,
    move_recv,
):
    grp = lax.axis_index("grp")
    seg = lax.axis_index("seg")
    me = grp * SEG + seg
    partner = (1 - grp) * SEG + seg
    own_lanes = pl.ds(0, LEAF)
    rows = COEF * NTYPES

    def load(source, target, k):
        copy = pltpu.make_async_copy(source, target, load_sem.at[k])
        copy.start()
        return copy

    loads = [
        load(coeffs_hbm, window.at[:, own_lanes], 0),
        load(up_hbm, up_op, 1),
        load(octant_hbm, leaf_octant, 2),
        load(tracer_hbm, tracers.at[:, own_lanes], 3),
        load(source_hbm, far_src, 4),
        load(type_hbm, far_type, 5),
        load(list_hbm, near_list, 6),
        load(kind_hbm, near_type, 7),
        load(owner_hbm, new_owner, 8),
        load(far_hbm, far_ops, 9),
        load(down_hbm, down_op, 10),
    ]
    chunks = []
    for k in range(CHUNKS):
        start = k * CHUNK
        part_of = pl.ds(start, min(CHUNK, rows - start))
        chunks.append(load(near_hbm.at[part_of], raw_ops.at[part_of], 11 + k))

    right = grp * SEG + lax.rem(seg + 1, SEG)
    left = grp * SEG + lax.rem(seg + SEG - 1, SEG)
    holder = jnp.where(lax.rem(me, 2) == 0, me + 1, lax.rem(me + SEG + 1, DEV))
    lister = jnp.where(lax.rem(me, 2) == 0, lax.rem(me + SEG - 1, DEV), me - 1)

    def on_line(j):
        return grp * SEG + (seg // LINE) * LINE + lax.rem(seg + j, LINE)

    def in_plane(j):
        return grp * SEG + lax.rem(seg + LINE * j, SEG)

    barrier = pltpu.get_barrier_semaphore()

    def greet(there):
        pl.semaphore_signal(barrier, inc=1, device_id=there, device_id_type=LOGICAL)

    greet(right)
    greet(left)
    for j in range(1, LINE):
        greet(on_line(j))
    greet(partner)
    greet(lister)

    def greet_plane(j, carry):
        greet(in_plane(j))
        return carry

    lax.fori_loop(1, PLANE, greet_plane, 0)

    for copy in loads[0:3]:
        copy.wait()
    leaf_pole = dot(up_op[...], window[:, 0:LEAF]).astype(BF)
    piece = hot(iota((16, LEAF), 0) == leaf_octant[...] - me * OCT_DEV)
    part = dot(piece, leaf_pole, 1, 1)
    ninth = part[8:9, :]
    part_row = iota((8, MULT), 0)
    lane_in = iota((MULT, 256), 0)
    lane_out = iota((MULT, 256), 1)
    spread = (
        (part[0:8, :], lane_out == lane_in),
        (jnp.where(part_row == 0, ninth, 0.0), (lane_out == lane_in + MULT) & (lane_in < CUT)),
        (jnp.where(part_row == 1, ninth, 0.0), (lane_out == lane_in + CUT_BACK) & (lane_in >= CUT)),
    )
    packed = jnp.zeros((8, 256), F32)
    for value, lanes in spread:
        packed = packed + dot(value.astype(BF), hot(lanes))
    poles[pl.ds(me, 1)] = packed.astype(BF)[None]

    loads[8].wait()
    owner_row = new_owner[...].astype(F32)
    leaf_row = iota((LEAF, LEAF), 0)
    leaf_col = iota((LEAF, LEAF), 1)
    owner = jnp.sum(jnp.where(leaf_row == leaf_col, owner_row, 0.0), axis=1, keepdims=True)
    before = (leaf_row < leaf_col) & (owner == owner_row)
    rank = jnp.sum(jnp.where(before, 1.0, 0.0), axis=0, keepdims=True)
    target = (owner_row * float(CAP) + rank).astype(I32)
    place[...] = hot(iota((DEV * CAP, LEAF), 0) == target)

    for copy in loads[3:6]:
        copy.wait()
    pl.semaphore_wait(barrier, GREETINGS)
    for j in range(1, LINE):
        remote(poles.at[me], poles.at[me], line_send, line_recv, on_line(j)).start()
    low = pl.ds(0, HALO)
    high = pl.ds(HALO, HALO)
    to_low = pl.ds(LEAF, HALO)
    to_high = pl.ds(LEAF + HALO, HALO)
    halos = [
        remote(src.at[:, lanes], src.at[:, there], halo_send.at[k], halo_recv.at[k], device)
        for k, (src, lanes, there, device) in enumerate(
            (
                (window, high, to_low, right),
                (window, low, to_high, left),
                (tracers, high, to_low, right),
                (tracers, low, to_high, left),
            )
        )
    ]
    lists = [
        remote(src, there, list_send.at[k], list_recv.at[k], device)
        for k, (src, there, device) in enumerate(
            (
                (far_src, source_in, holder),
                (far_type, type_in, holder),
                (far_src, source_edge, partner),
                (far_type, type_edge, partner),
            )
        )
    ]
    for copy in halos + lists:
        copy.start()

    for copy in loads[6:8]:
        copy.wait()
    listed = near_list[...]
    inside = (listed >= HALO) & (listed < HALO + LEAF)
    spot = jnp.where(inside, listed - HALO, jnp.where(listed < HALO, listed + LEAF, listed))
    kind = near_type[...]
    one = jnp.ones_like(kind)
    first_word = jnp.where(kind < 4, one << (8 * jnp.minimum(kind, 3)), 0)
    other_word = jnp.where(
        (kind >= 4) & (kind < NTYPES), one << (8 * (jnp.clip(kind, 4, 7) - 4)), 0
    )
    slots[0] = spot
    slots[1] = first_word
    slots[2] = other_word

    def count_rows(block, carry):
        base = pl.multiple_of(block * 32, 32)
        place_of = iota((32, LEAF), 0) + base
        first = jnp.zeros((32, LEAF), I32)
        other = jnp.zeros((32, LEAF), I32)
        for k in range(NEAR_K):
            here = place_of == slots[0, k : k + 1, :]
            first = first + jnp.where(here, slots[1, k : k + 1, :], 0)
            other = other + jnp.where(here, slots[2, k : k + 1, :], 0)
        for t in range(NTYPES):
            word = first if t < 4 else other
            value = lax.shift_right_logical(word, jnp.full_like(word, 8 * (t % 4))) & 255
            lanes = slice((t % 2) * LEAF, (t % 2 + 1) * LEAF)
            counts[t // 2, pl.ds(base, 32), lanes] = value.astype(F32).astype(BF)
        return carry

    lax.fori_loop(0, 16, count_rows, 0)

    all_line = remote(
        poles.at[pl.ds(0, LINE - 1)], poles.at[pl.ds(0, LINE - 1)], line_send, line_recv, partner
    )
    all_line.wait_recv()
    line = poles.at[pl.ds(grp * SEG + (seg // LINE) * LINE, LINE)]

    def send_line(j, carry):
        remote(line, line, plane_send, plane_recv, in_plane(j)).start()
        return carry

    lax.fori_loop(1, PLANE, send_line, 0)

    for copy in lists:
        copy.wait_recv()
    even = lax.rem(jnp.full((1, FAR_K), me, I32), 2) == 0
    lane = iota((FTYPES, OCTANTS), 1)
    for c in range(9):
        if c < OCT_DEV:
            source, kind_row = source_in[c : c + 1, :], type_in[c : c + 1, :]
        else:
            source = jnp.where(even, far_src[0:1, :], source_edge[0:1, :])
            kind_row = jnp.where(even, far_type[0:1, :], type_edge[0:1, :])
        source_hot = hot(iota((OCTANTS, FAR_K), 0) == source)
        kind_hot = hot(iota((FTYPES, FAR_K), 0) == kind_row)
        number = dot(kind_hot, source_hot, 1, 1)
        first = jnp.where(lax.rem(lane, 8) == 0, pltpu.roll(number, OCTANTS - 8, 1), 0.0)
        second = jnp.where(lax.rem(lane, 8) == 1, pltpu.roll(number, OCTANTS - 7, 1), 0.0)
        for k, value in enumerate((number, first, second)):
            at = k * TARGETS + c * FTYPES
            far_count[at : at + FTYPES, :] = value.astype(BF)

    raw_ops[rows : NBLK * 256, :] = jnp.zeros((NBLK * 256 - rows, COEF), BF)
    for t in range(NTYPES):
        ops[:, t * KPAD + 768 : (t + 1) * KPAD] = jnp.zeros((NBLK * OBLK, 128), BF)
        group[t * KPAD + 848 : (t + 1) * KPAD, :] = jnp.zeros((48, LEAF), BF)
    turn_row = iota((256, 256), 0)
    turn = hot(iota((256, 256), 1) == lax.rem(turn_row, OBLK) * NTYPES + turn_row // OBLK)
    for copy in loads[9:11]:
        copy.wait()

    def turn_blocks(b, carry):
        for part in range(3):
            at = b * 3 + part
            block = raw_ops[pl.ds(pl.multiple_of(at * 256, 256), 256), :]
            turned = dot(turn, block).astype(BF)
            out_rows = pl.ds(pl.multiple_of(at * OBLK, OBLK), OBLK)
            for t in range(NTYPES):
                ops[out_rows, t * KPAD : t * KPAD + COEF] = turned[t * OBLK : (t + 1) * OBLK, :]
        return carry

    for k, copy in enumerate(chunks):
        copy.wait()
        turn_blocks(k, 0)

    rest_of = pl.ds(0, SEG - LINE)
    all_plane = remote(poles.at[rest_of], poles.at[rest_of], plane_send, plane_recv, partner)
    all_plane.wait_recv()
    mine = poles.at[pl.ds(grp * SEG, SEG)]
    pair = remote(mine, mine, pair_send, pair_recv, partner)
    pair.start()

    for copy in halos:
        copy.wait_recv()

    def gather_kinds(two, carry):
        base = two * 2 * KPAD
        total = dot(window[...], counts[two]).astype(BF)
        group[pl.ds(base, COEF), :] = total[:, 0:LEAF]
        group[pl.ds(base + KPAD, COEF), :] = total[:, LEAF : 2 * LEAF]
        blend = dot(tracers[...], counts[two])
        mixed[two * 2, 0:NCOEF, :] = blend[:, 0:LEAF]
        mixed[two * 2 + 1, 0:NCOEF, :] = blend[:, LEAF : 2 * LEAF]
        return carry

    for two in range(NTYPES // 2):
        gather_kinds(two, 0)

    def near_rows(block, carry):
        here = pl.ds(pl.multiple_of(block * 320, 32), 320)
        velocity[here, :] = dot(ops[here, :], group[...])
        return carry

    lax.fori_loop(0, 2, near_rows, 0)

    pair.wait_recv()
    every = poles[...].astype(F32).reshape(OCTANTS, 256).astype(BF)
    sums = dot(far_count[...], every)
    lane = iota((TARGETS, 256), 1)
    first = pltpu.roll(sums[TARGETS : 2 * TARGETS], 256 - MULT, 1)
    second = pltpu.roll(sums[2 * TARGETS : 3 * TARGETS], 256 - CUT_BACK, 1)
    extra = jnp.where(lane < CUT, first, jnp.where(lane < MULT, second, 0.0))
    grouped = (sums[0:TARGETS] + extra).astype(BF)[:, 0:MULT]
    shifted = dot(far_ops[...], grouped, 1, 1)
    far_row = iota((MULT * FTYPES, TARGETS), 0)
    same = lax.rem(iota((MULT * FTYPES, TARGETS), 1), FTYPES) == lax.rem(far_row, FTYPES)
    shifted = jnp.where(same, shifted, 0.0).astype(BF)
    kinds = hot(iota((MULT, MULT * FTYPES), 1) // FTYPES == iota((MULT, MULT * FTYPES), 0))
    by_kind = dot(kinds, shifted).astype(BF)
    fold = hot(iota((16, TARGETS), 1) // FTYPES == iota((16, TARGETS), 0))
    nine = dot(fold, by_kind, 1, 1).astype(BF)
    leaf_local = dot(nine, piece, 0, 0).astype(BF)
    velocity[...] = velocity[...] + dot(down_op[:, 0:FRONT], leaf_local, 0, 0)

    message = dot(place[...], velocity[0:FRONT, :].astype(BF), 1, 1)
    front[...] = message.reshape(DEV, CAP, FRONT).astype(BF)

    def send_front(j, carry):
        there = lax.rem(me + j, DEV)
        remote(front.at[there], arrived_front.at[me], move_send.at[0], move_recv.at[0], there).start()
        return carry

    lax.fori_loop(1, DEV, send_front, 0)

    rest = dot(ops[FRONT : NBLK * OBLK, :], group[...])[0 : COEF - FRONT, :]
    rest = rest + dot(down_op[:, FRONT:COEF], leaf_local, 0, 0)

    flows = []
    total_in = jnp.zeros((1, LEAF), F32)
    for t in range(NTYPES):
        normal = (
            face_dirs[0, t] * velocity[0:1, :]
            + face_dirs[1, t] * velocity[NCOEF : NCOEF + 1, :]
            + face_dirs[2, t] * velocity[2 * NCOEF : 2 * NCOEF + 1, :]
        )
        number = jnp.sum(jnp.where(kind == t, 1.0, 0.0), axis=0, keepdims=True)
        flow = jnp.maximum(normal, 0.0)
        flows.append((flow, number))
        total_in = total_in + flow * number
    denominator = 1.0 + total_in
    kept = jnp.ones((1, LEAF), F32)
    blended = jnp.zeros((NCOEF, LEAF), F32)
    for t, (flow, number) in enumerate(flows):
        weight = flow / denominator
        kept = kept - weight * number
        blended = blended + mixed[t, 0:NCOEF, :] * weight
    blended = blended + tracers[:, 0:LEAF].astype(F32) * kept

    lower = jnp.concatenate([rest, blended, jnp.zeros((BACK - REST, LEAF), F32)], axis=0)
    message = dot(place[...], lower.astype(BF), 1, 1)
    back[...] = message.reshape(DEV, CAP, BACK).astype(BF)

    def send_back(j, carry):
        there = lax.rem(me + j, DEV)
        remote(back.at[there], arrived_back.at[me], move_send.at[1], move_recv.at[1], there).start()
        return carry

    lax.fori_loop(1, DEV, send_back, 0)
    arrived_front[pl.ds(me, 1)] = front[pl.ds(me, 1)]
    arrived_back[pl.ds(me, 1)] = back[pl.ds(me, 1)]

    for copy in halos + lists:
        copy.wait_send()
    all_line.wait_send()
    all_plane.wait_send()
    pair.wait_send()
    most = pl.ds(0, DEV - 1)
    for k, (sent, got) in enumerate(((front, arrived_front), (back, arrived_back))):
        last = remote(sent.at[most], got.at[most], move_send.at[k], move_recv.at[k], partner)
        last.wait_send()
        last.wait_recv()


def step(*args):
    (
        coeffs,
        tracer,
        up_op,
        far_ops,
        down_op,
        near_ops,
        face_dirs,
        leaf_octant,
        far_src,
        far_type,
        near_list,
        near_type,
        new_owner,
    ) = args
    whole = pl.BlockSpec(memory_space=VMEM)
    anywhere = pl.BlockSpec(memory_space=pl.ANY)
    dma = pltpu.SemaphoreType.DMA
    return pl.pallas_call(
        step_kernel,
        name="step",
        out_shape=(
            jax.ShapeDtypeStruct((DEV, CAP, FRONT), BF),
            jax.ShapeDtypeStruct((DEV, CAP, BACK), BF),
        ),
        in_specs=[anywhere] * 6 + [pl.BlockSpec(memory_space=pltpu.SMEM)] + [anywhere] * 6,
        out_specs=(whole, whole),
        scratch_shapes=[
            VMEM((COEF, 2 * LEAF), BF),
            VMEM((NCOEF, 2 * LEAF), BF),
            VMEM((MULT, COEF), BF),
            VMEM((MULT * FTYPES, MULT), BF),
            VMEM((MULT, COEF), BF),
            VMEM((1, LEAF), I32),
            VMEM((OCT_DEV, FAR_K), I32),
            VMEM((OCT_DEV, FAR_K), I32),
            VMEM((NEAR_K, LEAF), I32),
            VMEM((NEAR_K, LEAF), I32),
            VMEM((1, LEAF), I32),
            VMEM((NBLK * 256, COEF), BF),
            VMEM((NBLK * OBLK, NTYPES * KPAD), BF),
            VMEM((NTYPES // 2, 2 * LEAF, 2 * LEAF), BF),
            VMEM((NTYPES * KPAD, LEAF), BF),
            VMEM((NTYPES, 288, LEAF), F32),
            VMEM((DEV, 8, 256), BF),
            VMEM((3 * TARGETS, OCTANTS), BF),
            VMEM((OCT_DEV, FAR_K), I32),
            VMEM((OCT_DEV, FAR_K), I32),
            VMEM((OCT_DEV, FAR_K), I32),
            VMEM((OCT_DEV, FAR_K), I32),
            VMEM((DEV * CAP, LEAF), BF),
            VMEM((FRONT, LEAF), F32),
            VMEM((DEV, CAP, FRONT), BF),
            VMEM((DEV, CAP, BACK), BF),
            VMEM((3, NEAR_K, LEAF), I32),
            dma((11 + CHUNKS,)),
            dma((4,)),
            dma((4,)),
            dma((4,)),
            dma((4,)),
            dma,
            dma,
            dma,
            dma,
            dma,
            dma,
            dma((2,)),
            dma((2,)),
        ],
        compiler_params=pltpu.CompilerParams(
            collective_id=0, has_side_effects=True, vmem_limit_bytes=67_043_328
        ),
    )(
        coeffs,
        tracer,
        up_op,
        far_ops.reshape(MULT * FTYPES, MULT),
        down_op.T,
        near_ops.reshape(COEF * NTYPES, COEF),
        face_dirs,
        leaf_octant.reshape(1, LEAF),
        far_src.T,
        far_type.T,
        near_list,
        near_type,
        new_owner.reshape(1, LEAF),
    )


TURNS = ((0, 0, 384), (0, 384, 256), (1, 0, 256), (1, 256, 248))


def turn_kernel(front, back, moved, held, turned, in_sem, out_sem):
    loads = []
    for k, (which, start, count) in enumerate(TURNS):
        lanes = -(-count // 128) * 128
        source = (front, back)[which].at[:, :, pl.ds(start, lanes)]
        loads.append(
            pltpu.make_async_copy(source, held.at[k, :, :, pl.ds(0, lanes)], in_sem.at[k])
        )
    for copy in loads:
        copy.start()
    stores = []
    for k, (which, start, count) in enumerate(TURNS):
        loads[k].wait()
        lanes = -(-count // 128) * 128
        part = held[k, :, :, 0:lanes].astype(F32).reshape(DEV * CAP, lanes)
        turned[k, 0:lanes, :] = part.T.astype(BF)
        store = pltpu.make_async_copy(
            turned.at[k, pl.ds(0, count)],
            moved.at[pl.ds(which * FRONT + start, count)],
            out_sem.at[k],
        )
        store.start()
        stores.append(store)
    for copy in stores:
        copy.wait()


def local(*args):
    anywhere = pl.BlockSpec(memory_space=pl.ANY)
    return pl.pallas_call(
        turn_kernel,
        name="turn",
        out_shape=jax.ShapeDtypeStruct((COEF + NCOEF, DEV * CAP), BF),
        in_specs=[anywhere] * 2,
        out_specs=anywhere,
        scratch_shapes=[
            VMEM((4, DEV, CAP, 384), BF),
            VMEM((4, 384, DEV * CAP), BF),
            pltpu.SemaphoreType.DMA((4,)),
            pltpu.SemaphoreType.DMA((4,)),
        ],
    )(*step(*args))


def solution(mesh):
    split = P(None, GRP_SEG)
    in_specs = (
        split,
        split,
        P(),
        P(),
        P(),
        P(),
        P(),
        P(GRP_SEG),
        split,
        split,
        split,
        split,
        P(GRP_SEG, None),
    )
    return jax.shard_map(local, mesh=mesh, in_specs=in_specs, out_specs=split, check_vma=False)
```

```python
import functools

import jax
import jax.numpy as jnp
from jax import lax
from jax.experimental import pallas as pl
from jax.experimental.pallas import tpu as pltpu
from jax.sharding import PartitionSpec as P

NCOEF = 286
COEF = 858
MULT = 168
NTYPES = 8
NEAR_K = 27
FTYPES = 16
FAR_K = 189
LEAF = 256
HALO = 128
OCT_DEV = 8
OCTANTS = 1024
CAP = 4
SEG = 64
DEV = 128
KPAD = 896
OBLK = 32
NBLK = 27
FRONT = 640
BACK = 512
REST = 504
LINE = 4
PLANE = 16
TARGETS = 144
CUT = 88
CHUNKS = 9
CHUNK = 768
CUT_BACK = 80
GREETINGS = 22
GRP_SEG = ("grp", "seg")
LOGICAL = pl.DeviceIdType.LOGICAL
BF = jnp.bfloat16
F32 = jnp.float32
I32 = jnp.int32
VMEM = pltpu.VMEM


def dot(a, b, ca=1, cb=0):
    return lax.dot_general(a, b, (((ca,), (cb,)), ((), ())), preferred_element_type=F32)


def hot(mask):
    return jnp.where(mask, 1.0, 0.0).astype(BF)


def iota(shape, dim):
    return lax.broadcasted_iota(I32, shape, dim)


def remote(src, dst, send_sem, recv_sem, device):
    return pltpu.make_async_remote_copy(
        src_ref=src,
        dst_ref=dst,
        send_sem=send_sem,
        recv_sem=recv_sem,
        device_id=device,
        device_id_type=LOGICAL,
    )


def step_kernel(
    coeffs_hbm,
    tracer_hbm,
    up_hbm,
    far_hbm,
    down_hbm,
    near_hbm,
    face_dirs,
    octant_hbm,
    source_hbm,
    type_hbm,
    list_hbm,
    kind_hbm,
    owner_hbm,
    arrived_front,
    arrived_back,
    window,
    tracers,
    up_op,
    far_ops,
    down_op,
    leaf_octant,
    far_src,
    far_type,
    near_list,
    near_type,
    new_owner,
    raw_ops,
    ops,
    counts,
    group,
    mixed,
    poles,
    far_count,
    source_in,
    type_in,
    source_edge,
    type_edge,
    place,
    velocity,
    front,
    back,
    slots,
    load_sem,
    halo_send,
    halo_recv,
    list_send,
    list_recv,
    line_send,
    line_recv,
    plane_send,
    plane_recv,
    pair_send,
    pair_recv,
    move_send,
    move_recv,
):
    grp = lax.axis_index("grp")
    seg = lax.axis_index("seg")
    me = grp * SEG + seg
    partner = (1 - grp) * SEG + seg
    own_lanes = pl.ds(0, LEAF)
    rows = COEF * NTYPES

    def load(source, target, k):
        copy = pltpu.make_async_copy(source, target, load_sem.at[k])
        copy.start()
        return copy

    loads = [
        load(coeffs_hbm, window.at[:, own_lanes], 0),
        load(up_hbm, up_op, 1),
        load(octant_hbm, leaf_octant, 2),
        load(tracer_hbm, tracers.at[:, own_lanes], 3),
        load(source_hbm, far_src, 4),
        load(type_hbm, far_type, 5),
        load(list_hbm, near_list, 6),
        load(kind_hbm, near_type, 7),
        load(owner_hbm, new_owner, 8),
        load(far_hbm, far_ops, 9),
        load(down_hbm, down_op, 10),
    ]
    chunks = []
    for k in range(CHUNKS):
        start = k * CHUNK
        part_of = pl.ds(start, min(CHUNK, rows - start))
        chunks.append(load(near_hbm.at[part_of], raw_ops.at[part_of], 11 + k))

    right = grp * SEG + lax.rem(seg + 1, SEG)
    left = grp * SEG + lax.rem(seg + SEG - 1, SEG)
    holder = jnp.where(lax.rem(me, 2) == 0, me + 1, lax.rem(me + SEG + 1, DEV))
    lister = jnp.where(lax.rem(me, 2) == 0, lax.rem(me + SEG - 1, DEV), me - 1)

    def on_line(j):
        return grp * SEG + (seg // LINE) * LINE + lax.rem(seg + j, LINE)

    def in_plane(j):
        return grp * SEG + lax.rem(seg + LINE * j, SEG)

    barrier = pltpu.get_barrier_semaphore()

    def greet(there):
        pl.semaphore_signal(barrier, inc=1, device_id=there, device_id_type=LOGICAL)

    greet(right)
    greet(left)
    for j in range(1, LINE):
        greet(on_line(j))
    greet(partner)
    greet(lister)

    def greet_plane(j, carry):
        greet(in_plane(j))
        return carry

    lax.fori_loop(1, PLANE, greet_plane, 0)

    for copy in loads[0:3]:
        copy.wait()
    leaf_pole = dot(up_op[...], window[:, 0:LEAF]).astype(BF)
    piece = hot(iota((16, LEAF), 0) == leaf_octant[...] - me * OCT_DEV)
    part = dot(piece, leaf_pole, 1, 1)
    ninth = part[8:9, :]
    part_row = iota((8, MULT), 0)
    lane_in = iota((MULT, 256), 0)
    lane_out = iota((MULT, 256), 1)
    spread = (
        (part[0:8, :], lane_out == lane_in),
        (jnp.where(part_row == 0, ninth, 0.0), (lane_out == lane_in + MULT) & (lane_in < CUT)),
        (jnp.where(part_row == 1, ninth, 0.0), (lane_out == lane_in + CUT_BACK) & (lane_in >= CUT)),
    )
    packed = jnp.zeros((8, 256), F32)
    for value, lanes in spread:
        packed = packed + dot(value.astype(BF), hot(lanes))
    poles[pl.ds(me, 1)] = packed.astype(BF)[None]

    for copy in loads[3:6]:
        copy.wait()
    pl.semaphore_wait(barrier, GREETINGS)
    for j in range(1, LINE):
        remote(poles.at[me], poles.at[me], line_send, line_recv, on_line(j)).start()
    low = pl.ds(0, HALO)
    high = pl.ds(HALO, HALO)
    to_low = pl.ds(LEAF, HALO)
    to_high = pl.ds(LEAF + HALO, HALO)
    halos = [
        remote(src.at[:, lanes], src.at[:, there], halo_send.at[k], halo_recv.at[k], device)
        for k, (src, lanes, there, device) in enumerate(
            (
                (window, high, to_low, right),
                (window, low, to_high, left),
                (tracers, high, to_low, right),
                (tracers, low, to_high, left),
            )
        )
    ]
    lists = [
        remote(src, there, list_send.at[k], list_recv.at[k], device)
        for k, (src, there, device) in enumerate(
            (
                (far_src, source_in, holder),
                (far_type, type_in, holder),
                (far_src, source_edge, partner),
                (far_type, type_edge, partner),
            )
        )
    ]
    for copy in halos + lists:
        copy.start()

    for copy in loads[6:9]:
        copy.wait()
    listed = near_list[...]
    inside = (listed >= HALO) & (listed < HALO + LEAF)
    spot = jnp.where(inside, listed - HALO, jnp.where(listed < HALO, listed + LEAF, listed))
    kind = near_type[...]
    one = jnp.ones_like(kind)
    first_word = jnp.where(kind < 4, one << (8 * jnp.minimum(kind, 3)), 0)
    other_word = jnp.where(
        (kind >= 4) & (kind < NTYPES), one << (8 * (jnp.clip(kind, 4, 7) - 4)), 0
    )
    slots[0] = spot
    slots[1] = first_word
    slots[2] = other_word

    def count_rows(block, carry):
        base = pl.multiple_of(block * 32, 32)
        place_of = iota((32, LEAF), 0) + base
        first = jnp.zeros((32, LEAF), I32)
        other = jnp.zeros((32, LEAF), I32)
        for k in range(NEAR_K):
            here = place_of == slots[0, k : k + 1, :]
            first = first + jnp.where(here, slots[1, k : k + 1, :], 0)
            other = other + jnp.where(here, slots[2, k : k + 1, :], 0)
        for t in range(NTYPES):
            word = first if t < 4 else other
            value = lax.shift_right_logical(word, jnp.full_like(word, 8 * (t % 4))) & 255
            lanes = slice((t % 2) * LEAF, (t % 2 + 1) * LEAF)
            counts[t // 2, pl.ds(base, 32), lanes] = value.astype(F32).astype(BF)
        return carry

    lax.fori_loop(0, 16, count_rows, 0)

    all_line = remote(
        poles.at[pl.ds(0, LINE - 1)], poles.at[pl.ds(0, LINE - 1)], line_send, line_recv, partner
    )
    all_line.wait_recv()
    line = poles.at[pl.ds(grp * SEG + (seg // LINE) * LINE, LINE)]

    def send_line(j, carry):
        remote(line, line, plane_send, plane_recv, in_plane(j)).start()
        return carry

    lax.fori_loop(1, PLANE, send_line, 0)

    owner_row = new_owner[...].astype(F32)
    leaf_row = iota((LEAF, LEAF), 0)
    leaf_col = iota((LEAF, LEAF), 1)
    owner = jnp.sum(jnp.where(leaf_row == leaf_col, owner_row, 0.0), axis=1, keepdims=True)
    before = (leaf_row < leaf_col) & (owner == owner_row)
    rank = jnp.sum(jnp.where(before, 1.0, 0.0), axis=0, keepdims=True)
    target = (owner_row * float(CAP) + rank).astype(I32)
    place[...] = hot(iota((DEV * CAP, LEAF), 0) == target)

    for copy in lists:
        copy.wait_recv()
    even = lax.rem(jnp.full((1, FAR_K), me, I32), 2) == 0
    lane = iota((FTYPES, OCTANTS), 1)
    for c in range(9):
        if c < OCT_DEV:
            source, kind_row = source_in[c : c + 1, :], type_in[c : c + 1, :]
        else:
            source = jnp.where(even, far_src[0:1, :], source_edge[0:1, :])
            kind_row = jnp.where(even, far_type[0:1, :], type_edge[0:1, :])
        source_hot = hot(iota((OCTANTS, FAR_K), 0) == source)
        kind_hot = hot(iota((FTYPES, FAR_K), 0) == kind_row)
        number = dot(kind_hot, source_hot, 1, 1)
        first = jnp.where(lax.rem(lane, 8) == 0, pltpu.roll(number, OCTANTS - 8, 1), 0.0)
        second = jnp.where(lax.rem(lane, 8) == 1, pltpu.roll(number, OCTANTS - 7, 1), 0.0)
        for k, value in enumerate((number, first, second)):
            at = k * TARGETS + c * FTYPES
            far_count[at : at + FTYPES, :] = value.astype(BF)

    raw_ops[rows : NBLK * 256, :] = jnp.zeros((NBLK * 256 - rows, COEF), BF)
    for t in range(NTYPES):
        ops[:, t * KPAD + 768 : (t + 1) * KPAD] = jnp.zeros((NBLK * OBLK, 128), BF)
        group[t * KPAD + 848 : (t + 1) * KPAD, :] = jnp.zeros((48, LEAF), BF)
    turn_row = iota((256, 256), 0)
    turn = hot(iota((256, 256), 1) == lax.rem(turn_row, OBLK) * NTYPES + turn_row // OBLK)
    for copy in loads[9:11]:
        copy.wait()

    def turn_blocks(b, carry):
        for part in range(3):
            at = b * 3 + part
            block = raw_ops[pl.ds(pl.multiple_of(at * 256, 256), 256), :]
            turned = dot(turn, block).astype(BF)
            out_rows = pl.ds(pl.multiple_of(at * OBLK, OBLK), OBLK)
            for t in range(NTYPES):
                ops[out_rows, t * KPAD : t * KPAD + COEF] = turned[t * OBLK : (t + 1) * OBLK, :]
        return carry

    for k, copy in enumerate(chunks):
        copy.wait()
        turn_blocks(k, 0)

    rest_of = pl.ds(0, SEG - LINE)
    all_plane = remote(poles.at[rest_of], poles.at[rest_of], plane_send, plane_recv, partner)
    all_plane.wait_recv()
    mine = poles.at[pl.ds(grp * SEG, SEG)]
    pair = remote(mine, mine, pair_send, pair_recv, partner)
    pair.start()

    for copy in halos:
        copy.wait_recv()

    def gather_kinds(two, carry):
        base = two * 2 * KPAD
        total = dot(window[...], counts[two]).astype(BF)
        group[pl.ds(base, COEF), :] = total[:, 0:LEAF]
        group[pl.ds(base + KPAD, COEF), :] = total[:, LEAF : 2 * LEAF]
        blend = dot(tracers[...], counts[two])
        mixed[two * 2, 0:NCOEF, :] = blend[:, 0:LEAF]
        mixed[two * 2 + 1, 0:NCOEF, :] = blend[:, LEAF : 2 * LEAF]
        return carry

    for two in range(NTYPES // 2):
        gather_kinds(two, 0)

    def near_rows(block, carry):
        here = pl.ds(pl.multiple_of(block * 320, 32), 320)
        velocity[here, :] = dot(ops[here, :], group[...])
        return carry

    lax.fori_loop(0, 2, near_rows, 0)

    pair.wait_recv()
    every = poles[...].astype(F32).reshape(OCTANTS, 256).astype(BF)
    sums = dot(far_count[...], every)
    lane = iota((TARGETS, 256), 1)
    first = pltpu.roll(sums[TARGETS : 2 * TARGETS], 256 - MULT, 1)
    second = pltpu.roll(sums[2 * TARGETS : 3 * TARGETS], 256 - CUT_BACK, 1)
    extra = jnp.where(lane < CUT, first, jnp.where(lane < MULT, second, 0.0))
    grouped = (sums[0:TARGETS] + extra).astype(BF)[:, 0:MULT]
    shifted = dot(far_ops[...], grouped, 1, 1)
    far_row = iota((MULT * FTYPES, TARGETS), 0)
    same = lax.rem(iota((MULT * FTYPES, TARGETS), 1), FTYPES) == lax.rem(far_row, FTYPES)
    shifted = jnp.where(same, shifted, 0.0).astype(BF)
    kinds = hot(iota((MULT, MULT * FTYPES), 1) // FTYPES == iota((MULT, MULT * FTYPES), 0))
    by_kind = dot(kinds, shifted).astype(BF)
    fold = hot(iota((16, TARGETS), 1) // FTYPES == iota((16, TARGETS), 0))
    nine = dot(fold, by_kind, 1, 1).astype(BF)
    leaf_local = dot(nine, piece, 0, 0).astype(BF)
    velocity[...] = velocity[...] + dot(down_op[:, 0:FRONT], leaf_local, 0, 0)

    message = dot(place[...], velocity[0:FRONT, :].astype(BF), 1, 1)
    front[...] = message.reshape(DEV, CAP, FRONT).astype(BF)

    def send_front(j, carry):
        there = lax.rem(me + j, DEV)
        remote(front.at[there], arrived_front.at[me], move_send.at[0], move_recv.at[0], there).start()
        return carry

    lax.fori_loop(1, DEV, send_front, 0)

    rest = dot(ops[FRONT : NBLK * OBLK, :], group[...])[0 : COEF - FRONT, :]
    rest = rest + dot(down_op[:, FRONT:COEF], leaf_local, 0, 0)

    flows = []
    total_in = jnp.zeros((1, LEAF), F32)
    for t in range(NTYPES):
        normal = (
            face_dirs[0, t] * velocity[0:1, :]
            + face_dirs[1, t] * velocity[NCOEF : NCOEF + 1, :]
            + face_dirs[2, t] * velocity[2 * NCOEF : 2 * NCOEF + 1, :]
        )
        number = jnp.sum(jnp.where(kind == t, 1.0, 0.0), axis=0, keepdims=True)
        flow = jnp.maximum(normal, 0.0)
        flows.append((flow, number))
        total_in = total_in + flow * number
    denominator = 1.0 + total_in
    kept = jnp.ones((1, LEAF), F32)
    blended = jnp.zeros((NCOEF, LEAF), F32)
    for t, (flow, number) in enumerate(flows):
        weight = flow / denominator
        kept = kept - weight * number
        blended = blended + mixed[t, 0:NCOEF, :] * weight
    blended = blended + tracers[:, 0:LEAF].astype(F32) * kept

    lower = jnp.concatenate([rest, blended, jnp.zeros((BACK - REST, LEAF), F32)], axis=0)
    message = dot(place[...], lower.astype(BF), 1, 1)
    back[...] = message.reshape(DEV, CAP, BACK).astype(BF)

    def send_back(j, carry):
        there = lax.rem(me + j, DEV)
        remote(back.at[there], arrived_back.at[me], move_send.at[1], move_recv.at[1], there).start()
        return carry

    lax.fori_loop(1, DEV, send_back, 0)
    arrived_front[pl.ds(me, 1)] = front[pl.ds(me, 1)]
    arrived_back[pl.ds(me, 1)] = back[pl.ds(me, 1)]

    for copy in halos + lists:
        copy.wait_send()
    all_line.wait_send()
    all_plane.wait_send()
    pair.wait_send()
    most = pl.ds(0, DEV - 1)
    for k, (sent, got) in enumerate(((front, arrived_front), (back, arrived_back))):
        last = remote(sent.at[most], got.at[most], move_send.at[k], move_recv.at[k], partner)
        last.wait_send()
        last.wait_recv()


def step(*args):
    (
        coeffs,
        tracer,
        up_op,
        far_ops,
        down_op,
        near_ops,
        face_dirs,
        leaf_octant,
        far_src,
        far_type,
        near_list,
        near_type,
        new_owner,
    ) = args
    whole = pl.BlockSpec(memory_space=VMEM)
    anywhere = pl.BlockSpec(memory_space=pl.ANY)
    dma = pltpu.SemaphoreType.DMA
    return pl.pallas_call(
        step_kernel,
        name="step",
        out_shape=(
            jax.ShapeDtypeStruct((DEV, CAP, FRONT), BF),
            jax.ShapeDtypeStruct((DEV, CAP, BACK), BF),
        ),
        in_specs=[anywhere] * 6 + [pl.BlockSpec(memory_space=pltpu.SMEM)] + [anywhere] * 6,
        out_specs=(whole, whole),
        scratch_shapes=[
            VMEM((COEF, 2 * LEAF), BF),
            VMEM((NCOEF, 2 * LEAF), BF),
            VMEM((MULT, COEF), BF),
            VMEM((MULT * FTYPES, MULT), BF),
            VMEM((MULT, COEF), BF),
            VMEM((1, LEAF), I32),
            VMEM((OCT_DEV, FAR_K), I32),
            VMEM((OCT_DEV, FAR_K), I32),
            VMEM((NEAR_K, LEAF), I32),
            VMEM((NEAR_K, LEAF), I32),
            VMEM((1, LEAF), I32),
            VMEM((NBLK * 256, COEF), BF),
            VMEM((NBLK * OBLK, NTYPES * KPAD), BF),
            VMEM((NTYPES // 2, 2 * LEAF, 2 * LEAF), BF),
            VMEM((NTYPES * KPAD, LEAF), BF),
            VMEM((NTYPES, 288, LEAF), F32),
            VMEM((DEV, 8, 256), BF),
            VMEM((3 * TARGETS, OCTANTS), BF),
            VMEM((OCT_DEV, FAR_K), I32),
            VMEM((OCT_DEV, FAR_K), I32),
            VMEM((OCT_DEV, FAR_K), I32),
            VMEM((OCT_DEV, FAR_K), I32),
            VMEM((DEV * CAP, LEAF), BF),
            VMEM((FRONT, LEAF), F32),
            VMEM((DEV, CAP, FRONT), BF),
            VMEM((DEV, CAP, BACK), BF),
            VMEM((3, NEAR_K, LEAF), I32),
            dma((11 + CHUNKS,)),
            dma((4,)),
            dma((4,)),
            dma((4,)),
            dma((4,)),
            dma,
            dma,
            dma,
            dma,
            dma,
            dma,
            dma((2,)),
            dma((2,)),
        ],
        compiler_params=pltpu.CompilerParams(
            collective_id=0, has_side_effects=True, vmem_limit_bytes=67_043_328
        ),
    )(
        coeffs,
        tracer,
        up_op,
        far_ops.reshape(MULT * FTYPES, MULT),
        down_op.T,
        near_ops.reshape(COEF * NTYPES, COEF),
        face_dirs,
        leaf_octant.reshape(1, LEAF),
        far_src.T,
        far_type.T,
        near_list,
        near_type,
        new_owner.reshape(1, LEAF),
    )


TURNS = ((0, 0, 384), (0, 384, 256), (1, 0, 256), (1, 256, 248))


def turn_kernel(front, back, moved, held, turned, in_sem, out_sem):
    loads = []
    for k, (which, start, count) in enumerate(TURNS):
        lanes = -(-count // 128) * 128
        source = (front, back)[which].at[:, :, pl.ds(start, lanes)]
        loads.append(
            pltpu.make_async_copy(source, held.at[k, :, :, pl.ds(0, lanes)], in_sem.at[k])
        )
    for copy in loads:
        copy.start()
    stores = []
    for k, (which, start, count) in enumerate(TURNS):
        loads[k].wait()
        lanes = -(-count // 128) * 128
        part = held[k, :, :, 0:lanes].astype(F32).reshape(DEV * CAP, lanes)
        turned[k, 0:lanes, :] = part.T.astype(BF)
        store = pltpu.make_async_copy(
            turned.at[k, pl.ds(0, count)],
            moved.at[pl.ds(which * FRONT + start, count)],
            out_sem.at[k],
        )
        store.start()
        stores.append(store)
    for copy in stores:
        copy.wait()


def local(*args):
    anywhere = pl.BlockSpec(memory_space=pl.ANY)
    return pl.pallas_call(
        turn_kernel,
        name="turn",
        out_shape=jax.ShapeDtypeStruct((COEF + NCOEF, DEV * CAP), BF),
        in_specs=[anywhere] * 2,
        out_specs=anywhere,
        scratch_shapes=[
            VMEM((4, DEV, CAP, 384), BF),
            VMEM((4, 384, DEV * CAP), BF),
            pltpu.SemaphoreType.DMA((4,)),
            pltpu.SemaphoreType.DMA((4,)),
        ],
    )(*step(*args))


def solution(mesh):
    split = P(None, GRP_SEG)
    in_specs = (
        split,
        split,
        P(),
        P(),
        P(),
        P(),
        P(),
        P(GRP_SEG),
        split,
        split,
        split,
        split,
        P(GRP_SEG, None),
    )
    return jax.shard_map(local, mesh=mesh, in_specs=in_specs, out_specs=split, check_vma=False)
```
